32 devices in a mesh: dp: 2 (over y), row: 4 (over x, core), col: 4 (over z).
Axes of the slice: x: 2, y: 2, z: 4, core: 2. Of those that a mesh axis runs over, the one named last changes fastest.
Arguments:
- tokens: bfloat16 [2048, 8192], P(('dp', 'col'), 'row'), may hold values from -6 to 6
- frozen_weight: bfloat16 [8192, 8192], P('row', 'col'), may hold values from -0.0625 to 0.0625
- input_adapter_factor: bfloat16 [16, 8192], P(None, 'row'), may hold values from -0.0625 to 0.0625
- output_adapter_factor: bfloat16 [16, 8192], P(None, 'col'), may hold values from -1.5 to 1.5
- magnitude: float32 [8192], P('col'), may hold values from 0.5 to 2
- cotangent: bfloat16 [2048, 8192], P(('dp', 'row'), 'col'), may hold values from -6 to 6
- sequence_lengths: int32 [2, 8], P('dp'), may hold values from 1 to 512, 1024 in all within a row
Outputs:
- projected: bfloat16 [2048, 8192], P(('dp', 'row'), 'col')
- grad_mag: float32 [8192], P('col')
- input_factor_gradient: float32 [16, 8192], P(None, 'row')
- grad_b: float32 [16, 8192], P(None, 'col')
The draws below stay inside these ranges and needn't reach their ends.
Inputs may be any that keep to these rules, and one draw needn't show every extreme that they name: `sequence_lengths`: each group's 8 lengths sum to 1024, and one of them is exactly 512.
All inputs are finite; a program needn't handle non-finite values.
Results may differ from the reference program's by a relative error of at most 0.0052.
Values may be sent and summed in bfloat16 or wider, within the bound.
A program may use at most 64 MiB of HBM per device.

```python
import math
import jax
import jax.numpy as jnp
import numpy as np
from jax import lax

MODEL_WIDTH = 8192
ADAPTER_RANK = 16
TOK = 1024
SEQS = 8
LONGEST = 512
GROUPS = 2
TOKENS = 2048


def levels(stream_key, dims, cuts, least, largest):
    gain = 1.0
    for position, parts in cuts:
        heights = jax.random.uniform(jax.random.fold_in(jax.random.fold_in(stream_key, 6), position), (parts,), jnp.float32, least / len(cuts), largest / len(cuts))
        gain = gain * jnp.repeat(jnp.exp(heights), dims[position] // parts).reshape((-1,) + (1,) * (len(dims) - 1 - position))
    return gain


def length_profile(count, total, reach, lean):
    weights = [(1 << 20) // math.isqrt(rank ** lean) + 1 for rank in range(2, count + 1)]
    rest, holding = total - reach - (count - 1), [1] * (count - 1)
    while rest > 0:
        free = [i for i in range(count - 1) if holding[i] < reach]
        mass, left = sum([weights[i] for i in free]), rest
        for i in free:
            extra = min(reach - holding[i], max(1, left * weights[i] // mass), rest)
            holding[i] = holding[i] + extra
            rest = rest - extra
    return np.array([reach] + holding)


def uneven(rng, amount, total, limit, skew):
    if amount == 2:
        one = jax.random.randint(rng, (), max(1, total - limit), min(limit, total - 1) + 1)
        return jnp.stack([one, total - one])
    sizes = jnp.asarray(length_profile(amount, total, limit, skew), jnp.int32)
    couples = (amount - 1) // 2
    donor, sink = sizes[1:1 + 2 * couples:2], sizes[2:2 + 2 * couples:2]
    slack = jnp.minimum(donor - 1, limit - sink)
    shifted = jax.random.randint(jax.random.fold_in(rng, 1), (couples,), 0, 1 << 20) % (slack + 1)
    sizes = sizes.at[1:1 + 2 * couples:2].set(donor - shifted).at[2:2 + 2 * couples:2].set(sink + shifted)
    return sizes[jax.random.permutation(jax.random.fold_in(rng, 2), amount)]


def centred(own_key, shape, deviation, bound, pieces=(), held_as=jnp.bfloat16):
    gain = levels(own_key, shape, pieces, -0.22, 0.18) if pieces else 1.0
    result = jax.random.normal(own_key, shape, jnp.float32) * deviation * gain
    return jnp.minimum(jnp.maximum(result, -bound), bound).astype(held_as)


def setup_inputs(seed: int = 0) -> dict:
    keys = jax.random.split(jax.random.key(seed), 8)
    tokens = centred(keys[0], (TOKENS, MODEL_WIDTH), 1.0, 6.0, ((0, 8), (1, 4)))
    frozen_weight = centred(keys[1], (MODEL_WIDTH, MODEL_WIDTH), MODEL_WIDTH ** -0.5, 0.0625, ((0, 4), (1, 4)))
    input_adapter_factor = centred(keys[2], (ADAPTER_RANK, MODEL_WIDTH), MODEL_WIDTH ** -0.5, 0.0625, ((1, 4),))
    output_adapter_factor = centred(keys[3], (ADAPTER_RANK, MODEL_WIDTH), ADAPTER_RANK ** -0.5, 1.5, ((1, 4),))
    magnitude = jnp.clip(jnp.exp(math.log(2.0) - 1.3862944 * jax.random.uniform(keys[4], (MODEL_WIDTH,), jnp.float32) ** levels(keys[4], (MODEL_WIDTH,), ((0, 4),), -0.2, 0.2)), 0.5, 2.0)
    cotangent = centred(keys[5], (TOKENS, MODEL_WIDTH), 1.0, 6.0, ((0, 8), (1, 4)))
    sequence_lengths = jax.vmap(lambda own: uneven(own, SEQS, TOK, LONGEST, 2))(jax.random.split(keys[6], GROUPS)).reshape((GROUPS, SEQS)).astype(jnp.int32)
    return dict(tokens=tokens, frozen_weight=frozen_weight, input_adapter_factor=input_adapter_factor, output_adapter_factor=output_adapter_factor, magnitude=magnitude, cotangent=cotangent, sequence_lengths=sequence_lengths)


norm_eps = 1e-06
highest_precision = lax.Precision.HIGHEST

def contract_product(left, right, left_dim, right_dim):
    return lax.dot_general(left, right, (((left_dim,), (right_dim,)), ((), ())), preferred_element_type=jnp.float32)

def token_weights(lengths, positions):
    ends = jnp.cumsum(lengths, dtype=jnp.int32)
    starts = ends - lengths
    inside = (positions[:, None] >= starts[None, :]) & (positions[:, None] < ends[None, :])
    inverse = 1.0 / lengths.astype(jnp.float32)
    return lax.optimization_barrier(jnp.sum(jnp.where(inside, inverse[None, :], jnp.float32(0.0)), axis=1))

def reference(tokens, frozen_weight, input_adapter_factor, output_adapter_factor, magnitude, cotangent, sequence_lengths):
    low_rank_update = contract_product(input_adapter_factor, output_adapter_factor, 0, 0)
    merged = frozen_weight.astype(jnp.float32) + low_rank_update
    col_norm = jnp.sqrt(lax.optimization_barrier(jnp.sum(merged * merged, axis=0)) + norm_eps)
    col_scale = magnitude / col_norm
    down_activations = contract_product(tokens, input_adapter_factor, 1, 1).astype(jnp.bfloat16)
    query_projection = jnp.dot(tokens, frozen_weight, preferred_element_type=jnp.float32) + jnp.dot(down_activations, output_adapter_factor, preferred_element_type=jnp.float32)
    projected = (query_projection * col_scale[None, :]).astype(jnp.bfloat16)
    positions = jnp.arange(TOK, dtype=jnp.int32)
    weights = jax.vmap(lambda lengths: token_weights(lengths, positions))(sequence_lengths).reshape(-1)
    grad_out = cotangent.astype(jnp.float32) * weights[:, None]
    scale_grad = lax.optimization_barrier(jnp.sum(grad_out * query_projection, axis=0))
    grad_mag = scale_grad / col_norm
    norm_coefficient = -scale_grad * magnitude / (col_norm * col_norm * col_norm)
    projection_gradient = (grad_out * col_scale[None, :]).astype(jnp.bfloat16)
    gram_product_matrix = contract_product(input_adapter_factor, input_adapter_factor, 1, 1)
    merged_input_factor = jnp.dot(input_adapter_factor, frozen_weight, preferred_element_type=jnp.float32) + jnp.dot(gram_product_matrix, output_adapter_factor.astype(jnp.float32), precision=highest_precision)
    grad_b = contract_product(down_activations, projection_gradient, 0, 0) + merged_input_factor * norm_coefficient[None, :]
    backward_rows = contract_product(projection_gradient, output_adapter_factor, 1, 1).astype(jnp.bfloat16)
    scaled_output_factor = (output_adapter_factor.astype(jnp.float32) * norm_coefficient[None, :]).astype(jnp.bfloat16)
    input_factor_gradient = contract_product(backward_rows, tokens, 0, 0) + contract_product(scaled_output_factor, frozen_weight, 1, 1)
    input_factor_gradient = input_factor_gradient + jnp.dot(contract_product(scaled_output_factor, output_adapter_factor, 1, 1), input_adapter_factor.astype(jnp.float32), precision=highest_precision)
    return (projected, grad_mag, input_factor_gradient, grad_b)
```

```python
import functools

import jax
import jax.numpy as jnp
from jax import lax
from jax.experimental import pallas as pl
from jax.experimental.pallas import tpu as pltpu
from jax.sharding import PartitionSpec as P

norm_eps = 1e-06
highest_precision = lax.Precision.HIGHEST
MESH = pl.DeviceIdType.MESH
LANES = 128
FEATURE_TILE = 512
VMEM_LIMIT = 56 * 1024 * 1024


def contract_product(left, right, left_dim, right_dim):
    return lax.dot_general(
        left, right, (((left_dim,), (right_dim,)), ((), ())), preferred_element_type=jnp.float32
    )


def column_tiles(width, tile):
    return [(start, min(tile, width - start)) for start in range(0, width, tile)]


def adapter_kernel(
    D, C, R, S, L,
    tok, w_hbm, a_hbm, b_hbm, magnitude_hbm, cot_hbm, lengths,
    projected, grad_mag, factor_grad, grad_b,
    wx, gath, sb, pin, xin, pb, st_in, st_pair, a_ref, b_ref, magnitude, apad, bpad, acc, own_sum, pg, cot, late_cot,
    row_weight, late_weight, down_in, down_all, merged_factor, col_norm, col_scale, coefficient_scale,
    scale_in, back_in, back_rows, bsum, bsum_all, box1, fsum, fsum_in, message, line_in, line_out, end_out, end_in,
    load_sem, tok_sem, plane_sem, line_sem, gsend, grecv, ssend, precv, xrecv, stsend, strecv,
    dn_send, dn_recv, dz_send, dz_recv, late_send, late_recv, sc_send, sc_recv, bk_send, bk_recv,
    fs_send, fs_recv, ln_send, ln_recv, end_send, end_recv, r1a, r1b, r1c, r1d,
):
    z = lax.axis_index("col")
    r = lax.axis_index("row")
    d = lax.axis_index("dp")
    p, q = r // 2, r % 2
    pairs = R // 2
    sub, features = tok.shape[1], tok.shape[2]
    cols = w_hbm.shape[1]
    rank_rows = a_ref.shape[0]
    units = C * S
    block_units = units // R
    block_rows = block_units * sub
    chunks = block_units // S
    tiles = column_tiles(cols, 512)
    feature_tiles = column_tiles(features, FEATURE_TILE)
    f32, bf16 = jnp.float32, jnp.bfloat16
    half = units // 2
    catch_up = half + 3
    rate = 4

    g1 = D * R
    me1 = d * R + r

    def device1(i):
        peer = (me1 + i) % g1
        return {"dp": peer // R, "row": peer % R}

    def loop(n, body):
        def turn(i, carry):
            body(i)
            return carry

        lax.fori_loop(1, n, turn, 0)

    def remote(src, dst, send_sem, recv_sem, device):
        return pltpu.make_async_remote_copy(
            src_ref=src, dst_ref=dst, send_sem=send_sem, recv_sem=recv_sem,
            device_id=device, device_id_type=MESH,
        )

    def signal(sem, device):
        pl.semaphore_signal(sem, inc=1, device_id=device, device_id_type=MESH)

    def signal_line(sem):
        @pl.when(z > 0)
        def _():
            signal(sem, {"col": z - 1})

        @pl.when(z < C - 1)
        def _():
            signal(sem, {"col": z + 1})

    line_count = jnp.where(z > 0, 1, 0) + jnp.where(z < C - 1, 1, 0)

    barrier = pltpu.get_barrier_semaphore()
    signal_line(barrier)
    for i in range(1, R):
        signal(barrier, {"row": (r + i) % R})
    for i in range(1, D):
        signal(barrier, {"dp": (d + i) % D})

    def load_tok(s):
        return pltpu.make_async_copy(tok.at[s], gath.at[z * S + s], tok_sem.at[s])

    small_loads = [
        pltpu.make_async_copy(a_hbm, a_ref, load_sem.at[0]),
        pltpu.make_async_copy(b_hbm, b_ref, load_sem.at[1]),
        pltpu.make_async_copy(magnitude_hbm, magnitude, load_sem.at[2]),
    ]
    load_w = pltpu.make_async_copy(w_hbm, wx, load_sem.at[3])
    load_c = pltpu.make_async_copy(cot_hbm, cot, load_sem.at[4])
    for s in range(S):
        load_tok(s).start()
    for load in small_loads:
        load.start()
    load_w.start()
    load_c.start()

    pl.semaphore_wait(barrier, line_count + R - 1 + D - 1)

    def hop(u, direction):
        target = z - 1 if direction == 0 else z + 1
        return remote(gath.at[u], gath.at[u], gsend.at[direction, u], grecv.at[u], {"col": target})

    for s in range(S):
        load_tok(s).wait()

        @pl.when(z > 0)
        def _():
            hop(z * S + s, 0).start()

        @pl.when(z < C - 1)
        def _():
            hop(z * S + s, 1).start()

    for i in range(1, D):
        signal(plane_sem, {"dp": (d + i) % D})
    for load in small_loads:
        load.wait()

    def down_copy(i, piece):
        return remote(
            down_in.at[piece], down_in.at[piece], dn_send.at[i], dn_recv.at[i], {"row": (r + i) % R}
        )

    def spread_copy(i, piece):
        return remote(
            down_all.at[piece], down_all.at[piece], dz_send.at[i], dz_recv.at[i], {"col": (z + i) % C}
        )

    a = a_ref[...]
    own_tokens = gath[pl.ds(z * S, S)].reshape(S * sub, features)
    down_in[r] = contract_product(a, own_tokens, 1, 1)
    for i in range(1, R):
        down_copy(i, r).start()
    apad[...] = jnp.zeros_like(apad)
    bpad[...] = jnp.zeros_like(bpad)
    apad[0:rank_rows, :] = a
    bpad[0:rank_rows, :] = b_ref[...]
    if C > 2:
        signal_line(line_sem.at[0])

    far_chunk = jnp.where(z > C - 1 - z, 0, C - 1)
    late_first = far_chunk * S + S - L
    late_owner = late_first // block_units
    late_slot = late_first % block_units

    def weights_of(first, rows):
        position = first + lax.broadcasted_iota(jnp.int32, (rows, LANES), 0)
        weights = jnp.zeros((rows, LANES), f32)
        start_row = 0
        for i in range(lengths.shape[1]):
            length = lengths[0, i]
            end_row = start_row + length
            inverse = 1.0 / jnp.full((1, LANES), length, jnp.int32).astype(f32)
            weights = jnp.where((position >= start_row) & (position < end_row), inverse, weights)
            start_row = end_row
        return weights

    row_weight[...] = weights_of(r * block_rows, block_rows)
    late_weight[...] = weights_of(late_first * sub, L * sub)

    load_w.wait()

    gram = contract_product(a, a, 1, 1)
    for start, width in tiles:
        span = pl.ds(start, width)
        st_in[r, 0:rank_rows, span] = jnp.dot(
            a, wx[:, span], preferred_element_type=f32
        ) + jnp.dot(
            gram, b_ref[:, span].astype(f32),
            precision=highest_precision, preferred_element_type=f32,
        )
        st_in[r, rank_rows:rank_rows + 8, span] = jnp.zeros((8, width), f32)
    depth = 256

    def norm_step(i, carry):
        rows = pl.ds(pl.multiple_of(i * depth, depth), depth)
        for start, width in tiles:
            span = pl.ds(start, width)
            merged = wx[rows, span].astype(f32) + contract_product(apad[:, rows], bpad[:, span], 0, 0)
            st_in[r, rank_rows:rank_rows + 1, span] += jnp.sum(merged * merged, axis=0, keepdims=True)
        return carry

    lax.fori_loop(0, features // depth, norm_step, 0)

    partner = p * 2 + (1 - q)

    def stat_near():
        return remote(st_in.at[r], st_in.at[r], stsend.at[0], strecv.at[0], {"row": partner})

    def stat_far(i, piece):
        return remote(
            st_pair.at[piece], st_pair.at[piece], stsend.at[i], strecv.at[i],
            {"row": ((p + i) % pairs) * 2 + q},
        )

    stat_near().start()

    def pair_stats():
        remote(st_in.at[partner], st_in.at[partner], stsend.at[0], strecv.at[0], {"row": partner}).wait_recv()
        st_pair[p] = st_in[r] + st_in[partner]
        for i in range(1, pairs):
            stat_far(i, p).start()

    def greet():
        pl.semaphore_wait(line_sem.at[0], line_count)
        for i in range(1, C - 2):
            signal_line(line_sem.at[i])
            if i < C - 3:
                pl.semaphore_wait(line_sem.at[i], line_count)

    def spread_down():
        if C > 3:
            pl.semaphore_wait(line_sem.at[C - 3], line_count)
        for i in range(1, R):
            down_copy(i, (r - i + R) % R).wait_recv()
        down = down_in[0]
        for i in range(1, R):
            down = down + down_in[i]
        down_all[z] = down.astype(bf16)
        loop(C, lambda i: spread_copy(i, z).start())

    near = jnp.minimum(z, C - 1 - z)

    def place(k):
        j = k - S
        both = j < 2 * near * S
        rest = j - 2 * near * S
        distance = jnp.where(both, j // (2 * S) + 1, near + 1 + rest // S)
        s = jnp.where(both, (j % (2 * S)) // 2, rest % S)
        leftward = jnp.where(both, j % 2 == 0, z > C - 1 - z)
        chunk = jnp.where(leftward, z - distance, z + distance)
        own = k < S
        return jnp.where(own, z, chunk), jnp.where(own, k, s)

    def unit_of(k):
        c, s = place(k)
        return c * S + s

    def pair_copy(u):
        return remote(sb.at[u], pin.at[u], ssend.at[u], precv.at[u], {"row": p * 2 + (1 - q)})

    def far_copy(u, owner_pair):
        return remote(
            sb.at[u], xin.at[p, u % block_units], ssend.at[u], xrecv.at[p, u % block_units],
            {"row": owner_pair * 2 + q},
        )

    late_pair, late_core = late_owner // 2, late_owner % 2

    def late_far(i):
        rows = pl.ds(pl.multiple_of(late_slot * sub, sub), L * sub)
        return remote(cot.at[rows], late_cot, late_send.at[i], late_recv, {"row": ((p + i) % pairs) * 2 + q})

    def late_near():
        return remote(late_cot, late_cot, late_send.at[0], late_recv, {"row": partner})

    def back_copy(i, piece):
        return remote(back_in.at[piece], back_in.at[piece], bk_send.at[i], bk_recv.at[i], {"row": (r + i) % R})

    def scale_copy(i, piece):
        return remote(scale_in.at[piece], scale_in.at[piece], sc_send.at[i], sc_recv.at[i], device1(i))

    def group_sum(g, me, device, src, box, out, s1, r1, s2, r2):
        width = max(LANES, src.shape[1] // g)
        pieces = src.shape[1] // width

        def part(j):
            return pl.ds(pl.multiple_of(j * width, width), width)

        def scatter(i):
            return remote(src.at[:, part((me + i) % g % pieces)], box.at[i], s1.at[i], r1.at[i], device(i))

        def spread(i, j):
            return remote(out.at[:, part(j % pieces)], out.at[:, part(j % pieces)], s2.at[i], r2.at[i], device(i))

        def to_owner(i, action):
            @pl.when((me + i) % g < pieces)
            def _():
                action(scatter(i))

        def from_owner(i, action):
            @pl.when((me - i + g) % g < pieces)
            def _():
                action(spread(i, (me - i + g) % g))

        def begin():
            loop(g, lambda i: to_owner(i, lambda copy: copy.start()))

        def middle():
            @pl.when(me < pieces)
            def _():
                def add(i, total):
                    scatter(i).wait_recv()
                    return total + box[i]

                out[:, part(me % pieces)] = lax.fori_loop(1, g, add, src[:, part(me % pieces)])
                loop(g, lambda i: spread(i, me).start())

        def end():
            loop(g, lambda i: from_owner(i, lambda copy: copy.wait_recv()))

        def drain():
            loop(g, lambda i: to_owner(i, lambda copy: copy.wait_send()))

            @pl.when(me < pieces)
            def _():
                loop(g, lambda i: spread(i, me).wait_send())

        return begin, middle, end, drain

    begin1, middle1, end1, drain1 = group_sum(
        g1, me1, device1, bsum, box1, bsum_all, r1a, r1b, r1c, r1d
    )

    def early():
        for i in range(1, pairs):
            stat_far(i, (p - i + pairs) % pairs).wait_recv()
        stats = st_pair[0]
        for i in range(1, pairs):
            stats = stats + st_pair[i]
        merged_factor[...] = stats[0:rank_rows]
        norm = jnp.sqrt(stats[rank_rows:rank_rows + 1] + norm_eps)
        col_norm[...] = norm
        col_scale[...] = magnitude[...] / norm
        coefficient_scale[...] = -magnitude[...] / (norm * norm * norm)
        load_c.wait()
        scale_in[me1] = jnp.zeros((1, cols), f32)
        for v in range(block_units):
            rows = pl.ds(v * sub, sub)
            weight = row_weight[rows, 0:1]
            for start, width in tiles:
                span = pl.ds(start, width)
                grad_out = cot[rows, span].astype(f32) * weight
                pg[rows, span] = (grad_out * col_scale[:, span]).astype(bf16)
        back_in[r] = contract_product(b_ref[...], pg[...], 1, 1).astype(bf16)
        for i in range(1, R):
            back_copy(i, r).start()

    def middle():
        loop(C, lambda i: spread_copy(i, (z - i + C) % C).wait_recv())
        for start, width in tiles:
            span = pl.ds(start, width)
            total = jnp.zeros((rank_rows, width), f32)
            for i in range(chunks):
                down = down_all[r * chunks + i]
                total = total + jnp.dot(
                    down, pg[i * S * sub:(i + 1) * S * sub, span], preferred_element_type=f32
                )
                acc[i * S:(i + 1) * S, :, span] = contract_product(
                    down, b_ref[:, span], 0, 0
                ).reshape(S, sub, width)
            bsum[:, span] = total
        if D > 1:
            pl.semaphore_wait(plane_sem, D - 1)
        begin1()

        @pl.when(r == late_owner)
        def _():
            for i in range(L):
                rows = pl.ds(pl.multiple_of((late_slot + i) * sub, sub), sub)
                weight = row_weight[rows, 0:1]
                for start, width in tiles:
                    span = pl.ds(start, width)
                    grad_out = cot[rows, span].astype(f32) * weight
                    scale_in[me1, :, span] += jnp.sum(
                        grad_out * acc[late_slot + i, :, span], axis=0, keepdims=True
                    )

    def send_late():
        @pl.when(r == late_owner)
        def _():
            for i in range(1, pairs):
                late_far(i).start()
            late_cot[...] = cot[pl.ds(pl.multiple_of(late_slot * sub, sub), L * sub), :]

    def pass_late():
        @pl.when(q == late_core)
        def _():
            @pl.when(p != late_pair)
            def _():
                late_near().wait_recv()

            late_near().start()

    def multiply(k):
        c, s = place(k)
        u = c * S + s
        owner = u // block_units

        @pl.when(k >= S)
        def _():
            hop(u, 0).wait_recv()

            @pl.when((c < z) & (z < C - 1))
            def _():
                hop(u, 1).start()

            @pl.when((c > z) & (z > 0))
            def _():
                hop(u, 0).start()

        slot = k % 2
        for start, width in tiles:
            span = pl.ds(start, width)
            pb[slot, :, span] = jnp.dot(gath[u], wx[:, span], preferred_element_type=f32)

        @pl.when(k >= units - L)
        def _():
            @pl.when((k == units - L) & (q != late_core))
            def _():
                late_near().wait_recv()

            rows = pl.ds(pl.multiple_of((k - units + L) * sub, sub), sub)
            weight = late_weight[rows, 0:1]
            for start, width in tiles:
                span = pl.ds(start, width)
                grad_out = late_cot[rows, span].astype(f32) * weight
                scale_in[me1, :, span] += jnp.sum(grad_out * pb[slot, :, span], axis=0, keepdims=True)

        @pl.when(k == units - 1)
        def _():
            loop(g1, lambda i: scale_copy(i, me1).start())

        @pl.when(owner % 2 != q)
        def _():
            sb[u] = pb[slot].astype(bf16)
            pair_copy(u).start()

    def combine(k):
        u = unit_of(k)
        owner = u // block_units
        slot = k % 2

        @pl.when(owner % 2 == q)
        def _():
            pair_copy(u).wait_recv()
            total = pb[slot] + pin[u].astype(f32)

            @pl.when(owner // 2 == p)
            def _():
                own_sum[u % block_units] = total

            @pl.when(owner // 2 != p)
            def _():
                sb[u] = total.astype(bf16)
                far_copy(u, owner // 2).start()

    def factor_term(k):
        u = unit_of(k)
        block = u // block_units
        rows = pl.ds(pl.multiple_of((u % block_units) * sub, sub), sub)
        back = back_rows[block, rows, :]
        for start, width in feature_tiles:
            span = pl.ds(start, width)
            fsum[:, span] += contract_product(back, gath[u, :, span], 0, 0)[0:rank_rows]

    def finish(k):
        u = unit_of(k)

        @pl.when(u // block_units == r)
        def _():
            v = u % block_units
            for i in range(1, pairs):
                other = (p + i) % pairs
                remote(
                    sb.at[v], xin.at[other, v], ssend.at[v], xrecv.at[other, v], {"row": other * 2 + q}
                ).wait_recv()
            rows = pl.ds(pl.multiple_of(v * sub, sub), sub)
            weight = row_weight[rows, 0:1]
            for start, width in tiles:
                span = pl.ds(start, width)
                query = acc[v, :, span] + own_sum[v, :, span]
                for i in range(1, pairs):
                    query = query + xin[(p + i) % pairs, v, :, span].astype(f32)
                projected[rows, span] = (query * col_scale[:, span]).astype(bf16)
                grad_out = cot[rows, span].astype(f32) * weight

                @pl.when(k < units - L)
                def _():
                    scale_in[me1, :, span] += jnp.sum(grad_out * query, axis=0, keepdims=True)

    def each(first, last, body):
        def turn(i, carry):
            body(i)
            return carry

        lax.fori_loop(first, last, turn, 0)

    fsum[...] = jnp.zeros_like(fsum)

    def step(k, carry):
        @pl.when(k > 0)
        def _():
            combine(k - 1)

        @pl.when(k == 1)
        def _():
            pair_stats()

        if C > 2:
            @pl.when(k == 2)
            def _():
                greet()

        @pl.when(k == S)
        def _():
            spread_down()

        @pl.when(k == half)
        def _():
            early()

        @pl.when(k == half + 1)
        def _():
            send_late()

        @pl.when(k == half + 2)
        def _():
            middle()

        @pl.when(k == catch_up)
        def _():
            for i in range(1, R):
                back_copy(i, (r - i + R) % R).wait_recv()
            one = (
                lax.broadcasted_iota(jnp.int32, (rank_rows, LANES), 0)
                == lax.broadcasted_iota(jnp.int32, (rank_rows, LANES), 1)
            ).astype(f32).astype(bf16)
            for j in range(R):
                back_rows[j] = contract_product(back_in[j], one, 0, 0).astype(bf16)

        @pl.when(k >= catch_up)
        def _():
            done = rate * (k - catch_up)
            each(jnp.minimum(done, k - 1), jnp.minimum(done + rate, k), factor_term)
            each(jnp.minimum(done, k - 2), jnp.minimum(done + rate, k - 1), finish)

        @pl.when(k == catch_up + 1)
        def _():
            pass_late()

        @pl.when(k == units - 2)
        def _():
            middle1()

        multiply(k)
        return carry

    lax.fori_loop(0, units, step, 0)

    factor_term(units - 1)

    def group_copy(i, piece):
        return remote(fsum_in.at[piece], fsum_in.at[piece], fs_send.at[i], fs_recv.at[i], {"dp": (d + i) % D})

    fsum_in[d] = fsum[...].astype(bf16)
    for i in range(1, D):
        group_copy(i, d).start()
    combine(units - 1)

    ends = (z == 0) | (z == C - 1)
    side = jnp.where(z == 0, 0, 1)

    def end_copy(i, t):
        target = jnp.where(z == 0, i, C - 1 - i)
        return remote(end_out.at[t], end_in.at[side, t], end_send.at[i, t], end_recv.at[side, t], {"col": target})

    def end_arrived(j):
        for t, (start, width) in enumerate(feature_tiles):
            span = pl.ds(start, width)
            remote(
                end_out.at[t], end_in.at[j, t], end_send.at[0, t], end_recv.at[j, t], {"col": (z + 1) % C}
            ).wait_recv()
            message[:, span] += end_in[j, t].astype(f32)

    def line_copy(direction):
        target = z - 1 if direction == 0 else z + 1
        return remote(
            line_out.at[direction], line_in.at[direction], ln_send.at[direction], ln_recv.at[direction],
            {"col": target},
        )

    loop(g1, lambda i: scale_copy(i, (me1 - i + g1) % g1).wait_recv())
    scale_grad = scale_in[0]
    for j in range(1, g1):
        scale_grad = scale_grad + scale_in[j]
    coefficient = scale_grad * coefficient_scale[...]
    scaled = (b_ref[...].astype(f32) * coefficient).astype(bf16)
    cross = contract_product(scaled, b_ref[...], 1, 1)
    for t, (start, width) in enumerate(feature_tiles):
        span = pl.ds(start, width)
        total = contract_product(scaled, wx[span, :], 1, 1) + jnp.dot(
            cross, a_ref[:, span].astype(f32),
            precision=highest_precision, preferred_element_type=f32,
        )
        total = total + fsum[:, span]
        if t == 0:
            for i in range(1, D):
                group_copy(i, (d - i + D) % D).wait_recv()
        for i in range(1, D):
            total = total + fsum_in[(d - i + D) % D, :, span].astype(f32)
        message[:, span] = total

        @pl.when(ends)
        def _():
            end_out[t] = message[:, span].astype(bf16)
            for i in range(C - 1, 0, -1):
                end_copy(i, t).start()

    if C > 2:
        @pl.when((z > 0) & (z < C - 1))
        def _():
            own = message[...]
            for direction in (0, 1):
                more = (z < C - 2) if direction == 0 else (z > 1)

                @pl.when(more)
                def _():
                    line_copy(direction).wait_recv()
                    incoming = line_in[direction].astype(f32)
                    line_out[direction] = (own + incoming).astype(bf16)
                    message[...] += incoming

                @pl.when(jnp.logical_not(more))
                def _():
                    line_out[direction] = own.astype(bf16)

                line_copy(direction).start()

    each(units - 2, units, finish)
    grad_mag[...] = scale_grad / col_norm[...]
    end1()
    grad_b[...] = bsum_all[...] + merged_factor[...] * coefficient

    drain1()
    loop(g1, lambda i: scale_copy(i, me1).wait_send())
    for i in range(1, R):
        back_copy(i, r).wait_send()
        down_copy(i, r).wait_send()
    loop(C, lambda i: spread_copy(i, z).wait_send())
    for i in range(1, D):
        group_copy(i, d).wait_send()

    stat_near().wait_send()
    for i in range(1, pairs):
        stat_far(i, p).wait_send()

    @pl.when(r == late_owner)
    def _():
        for i in range(1, pairs):
            late_far(i).wait_send()

    @pl.when(q == late_core)
    def _():
        late_near().wait_send()

    def drain(u, carry):
        c = u // S
        owner = u // block_units

        @pl.when((owner % 2 != q) | (owner // 2 != p))
        def _():
            pair_copy(u).wait_send()

        @pl.when((c <= z) & (z < C - 1))
        def _():
            hop(u, 1).wait_send()

        @pl.when((c >= z) & (z > 0))
        def _():
            hop(u, 0).wait_send()

        return carry

    lax.fori_loop(0, units, drain, 0)

    if C > 2:
        @pl.when(z == 0)
        def _():
            line_copy(0).wait_recv()
            message[...] += line_in[0].astype(f32)

        @pl.when(z == C - 1)
        def _():
            line_copy(1).wait_recv()
            message[...] += line_in[1].astype(f32)

    @pl.when(z > 0)
    def _():
        end_arrived(0)

    @pl.when(z < C - 1)
    def _():
        end_arrived(1)

    factor_grad[...] = message[...]

    @pl.when(ends)
    def _():
        for t in range(len(feature_tiles)):
            for i in range(C - 1, 0, -1):
                end_copy(i, t).wait_send()

    if C > 2:
        @pl.when((z > 0) & (z < C - 1))
        def _():
            line_copy(0).wait_send()
            line_copy(1).wait_send()


def per_device(
    tokens,
    frozen_weight,
    input_adapter_factor,
    output_adapter_factor,
    magnitude,
    cotangent,
    sequence_lengths,
):
    D, C, R = lax.axis_size("dp"), lax.axis_size("col"), lax.axis_size("row")
    local_rows, features = tokens.shape
    block_rows, cols = cotangent.shape
    rank_rows = input_adapter_factor.shape[0]
    S, L = 4, 2
    feature_tiles = features // FEATURE_TILE
    sub = local_rows // S
    units = C * S
    block_units = units // R
    g1 = D * R
    vmem = pl.BlockSpec(memory_space=pltpu.VMEM)
    smem = pl.BlockSpec(memory_space=pltpu.SMEM)
    hbm = pl.BlockSpec(memory_space=pl.ANY)
    dma = pltpu.SemaphoreType.DMA
    regular = pltpu.SemaphoreType.REGULAR
    f32, bf16 = jnp.float32, jnp.bfloat16
    projected, grad_mag, factor_grad, grad_b = pl.pallas_call(
        functools.partial(adapter_kernel, D, C, R, S, L),
        out_shape=(
            pltpu.VMEM((block_rows, cols), bf16),
            pltpu.VMEM((1, cols), f32),
            pltpu.VMEM((rank_rows, features), f32),
            pltpu.VMEM((rank_rows, cols), f32),
        ),
        in_specs=[hbm, hbm, hbm, hbm, hbm, hbm, smem],
        out_specs=(vmem, vmem, vmem, vmem),
        scratch_shapes=[
            pltpu.VMEM((features, cols), bf16),
            pltpu.VMEM((units, sub, features), bf16),
            pltpu.VMEM((units, sub, cols), bf16),
            pltpu.VMEM((units, sub, cols), bf16),
            pltpu.VMEM((R // 2, block_units, sub, cols), bf16),
            pltpu.VMEM((2, sub, cols), f32),
            pltpu.VMEM((R, rank_rows + 8, cols), f32),
            pltpu.VMEM((R // 2, rank_rows + 8, cols), f32),
            pltpu.VMEM((rank_rows, features), bf16),
            pltpu.VMEM((rank_rows, cols), bf16),
            pltpu.VMEM((1, cols), f32),
            pltpu.VMEM((LANES, features), bf16),
            pltpu.VMEM((LANES, cols), bf16),
            pltpu.VMEM((block_units, sub, cols), f32),
            pltpu.VMEM((block_units, sub, cols), f32),
            pltpu.VMEM((block_rows, cols), bf16),
            pltpu.VMEM((block_rows, cols), bf16),
            pltpu.VMEM((L * sub, cols), bf16),
            pltpu.VMEM((block_rows, LANES), f32),
            pltpu.VMEM((L * sub, LANES), f32),
            pltpu.VMEM((R, rank_rows, local_rows), f32),
            pltpu.VMEM((C, rank_rows, local_rows), bf16),
            pltpu.VMEM((rank_rows, cols), f32),
            pltpu.VMEM((1, cols), f32),
            pltpu.VMEM((1, cols), f32),
            pltpu.VMEM((1, cols), f32),
            pltpu.VMEM((g1, 1, cols), f32),
            pltpu.VMEM((R, rank_rows, block_rows), bf16),
            pltpu.VMEM((R, block_rows, LANES), bf16),
            pltpu.VMEM((rank_rows, cols), f32),
            pltpu.VMEM((rank_rows, cols), f32),
            pltpu.VMEM((g1, rank_rows, max(LANES, cols // g1)), f32),
            pltpu.VMEM((rank_rows, features), f32),
            pltpu.VMEM((D, rank_rows, features), bf16),
            pltpu.VMEM((rank_rows, features), f32),
            pltpu.VMEM((2, rank_rows, features), bf16),
            pltpu.VMEM((2, rank_rows, features), bf16),
            pltpu.VMEM((feature_tiles, rank_rows, features // feature_tiles), bf16),
            pltpu.VMEM((2, feature_tiles, rank_rows, features // feature_tiles), bf16),
            dma((5,)),
            dma((S,)),
            regular,
            pltpu.SemaphoreType.REGULAR((max(1, C - 2),)),
            dma((2, units)),
            dma((units,)),
            dma((units,)),
            dma((units,)),
            dma((R // 2, block_units)),
            dma((R,)),
            dma((R,)),
            dma((R,)),
            dma((R,)),
            dma((C,)),
            dma((C,)),
            dma((R,)),
            dma(()),
            dma((g1,)),
            dma((g1,)),
            dma((R,)),
            dma((R,)),
            dma((D,)),
            dma((D,)),
            dma((2,)),
            dma((2,)),
            dma((C, feature_tiles)),
            dma((2, feature_tiles)),
        ] + [dma((g1,))] * 4,
        compiler_params=pltpu.CompilerParams(
            collective_id=0, has_side_effects=True, vmem_limit_bytes=VMEM_LIMIT
        ),
    )(
        tokens.reshape(S, sub, features), frozen_weight, input_adapter_factor,
        output_adapter_factor, magnitude.reshape(1, cols), cotangent, sequence_lengths,
    )
    return projected, grad_mag.reshape(cols), factor_grad, grad_b


def solution(mesh):
    in_specs = (
        P(("dp", "col"), "row"),
        P("row", "col"),
        P(None, "row"),
        P(None, "col"),
        P("col"),
        P(("dp", "row"), "col"),
        P("dp", None),
    )
    out_specs = (P(("dp", "row"), "col"), P("col"), P(None, "row"), P(None, "col"))
    return jax.shard_map(
        per_device, mesh=mesh, in_specs=in_specs, out_specs=out_specs, check_vma=False
    )
```

```python
import functools

import jax
import jax.numpy as jnp
from jax import lax
from jax.experimental import pallas as pl
from jax.experimental.pallas import tpu as pltpu
from jax.sharding import PartitionSpec as P

norm_eps = 1e-06
highest_precision = lax.Precision.HIGHEST
MESH = pl.DeviceIdType.MESH
LANES = 128
FEATURE_TILE = 512
VMEM_LIMIT = 56 * 1024 * 1024


def contract_product(left, right, left_dim, right_dim):
    return lax.dot_general(
        left, right, (((left_dim,), (right_dim,)), ((), ())), preferred_element_type=jnp.float32
    )


def column_tiles(width, tile):
    return [(start, min(tile, width - start)) for start in range(0, width, tile)]


def adapter_kernel(
    D, C, R, S, L,
    tok, w_hbm, a_hbm, b_hbm, magnitude_hbm, cot_hbm, lengths_hbm,
    projected, grad_mag, factor_grad, grad_b,
    lengths, wx, gath, sb, pin, xin, pb, st_in, st_pair, a_ref, b_ref, magnitude, apad, bpad, acc, own_sum, pg, cot, late_cot,
    row_weight, late_weight, down_in, down_all, merged_factor, col_norm, col_scale, coefficient_scale,
    scale_in, back_in, back_rows, bsum, bsum_all, box1, fsum, fsum_in, message, line_in, line_out, end_out, end_in,
    load_sem, tok_sem, plane_sem, line_sem, gsend, grecv, ssend, precv, xrecv, stsend, strecv,
    dn_send, dn_recv, dz_send, dz_recv, late_send, late_recv, sc_send, sc_recv, bk_send, bk_recv,
    fs_send, fs_recv, ln_send, ln_recv, end_send, end_recv, r1a, r1b, r1c, r1d,
):
    z = lax.axis_index("col")
    r = lax.axis_index("row")
    d = lax.axis_index("dp")
    p, q = r // 2, r % 2
    pairs = R // 2
    sub, features = tok.shape[1], tok.shape[2]
    cols = w_hbm.shape[1]
    rank_rows = a_ref.shape[0]
    units = C * S
    block_units = units // R
    block_rows = block_units * sub
    chunks = block_units // S
    tiles = column_tiles(cols, 512)
    feature_tiles = column_tiles(features, FEATURE_TILE)
    f32, bf16 = jnp.float32, jnp.bfloat16
    half = units // 2
    catch_up = half + 3
    rate = 4

    g1 = D * R
    me1 = d * R + r

    def device1(i):
        peer = (me1 + i) % g1
        return {"dp": peer // R, "row": peer % R}

    def loop(n, body):
        def turn(i, carry):
            body(i)
            return carry

        lax.fori_loop(1, n, turn, 0)

    def remote(src, dst, send_sem, recv_sem, device):
        return pltpu.make_async_remote_copy(
            src_ref=src, dst_ref=dst, send_sem=send_sem, recv_sem=recv_sem,
            device_id=device, device_id_type=MESH,
        )

    def settle(view, sem, device):
        return remote(view, view, sem, sem, device)

    def signal(sem, device):
        pl.semaphore_signal(sem, inc=1, device_id=device, device_id_type=MESH)

    def signal_line(sem):
        @pl.when(z > 0)
        def _():
            signal(sem, {"col": z - 1})

        @pl.when(z < C - 1)
        def _():
            signal(sem, {"col": z + 1})

    line_count = jnp.where(z > 0, 1, 0) + jnp.where(z < C - 1, 1, 0)

    barrier = pltpu.get_barrier_semaphore()
    signal_line(barrier)
    for i in range(1, R):
        signal(barrier, {"row": (r + i) % R})
    for i in range(1, D):
        signal(barrier, {"dp": (d + i) % D})

    def load_tok(s):
        return pltpu.make_async_copy(tok.at[s], gath.at[z * S + s], tok_sem.at[s])

    small_loads = [
        pltpu.make_async_copy(a_hbm, a_ref, load_sem.at[0]),
        pltpu.make_async_copy(b_hbm, b_ref, load_sem.at[1]),
        pltpu.make_async_copy(magnitude_hbm, magnitude, load_sem.at[2]),
        pltpu.make_async_copy(lengths_hbm, lengths, load_sem.at[5]),
    ]
    load_w = pltpu.make_async_copy(w_hbm, wx, load_sem.at[3])
    load_c = pltpu.make_async_copy(cot_hbm, cot, load_sem.at[4])
    for s in range(S):
        load_tok(s).start()
    for load in small_loads:
        load.start()
    load_w.start()
    load_c.start()

    pl.semaphore_wait(barrier, line_count + R - 1 + D - 1)

    def hop(u, direction):
        target = z - 1 if direction == 0 else z + 1
        slot = u if direction == 0 else jnp.where(u // S == z, units + u % S, u)
        return remote(gath.at[u], gath.at[u], gsend.at[slot], grecv.at[u], {"col": target})

    for s in range(S):
        load_tok(s).wait()

        @pl.when(z > 0)
        def _():
            hop(z * S + s, 0).start()

        @pl.when(z < C - 1)
        def _():
            hop(z * S + s, 1).start()

    for i in range(1, D):
        signal(plane_sem, {"dp": (d + i) % D})
    for load in small_loads:
        load.wait()

    def down_copy(i, piece):
        return remote(
            down_in.at[piece], down_in.at[piece], dn_send, dn_recv, {"row": (r + i) % R}
        )

    def spread_copy(i, piece):
        return remote(
            down_all.at[piece], down_all.at[piece], dz_send, dz_recv, {"col": (z + i) % C}
        )

    a = a_ref[...]
    own_tokens = gath[pl.ds(z * S, S)].reshape(S * sub, features)
    down_in[r] = contract_product(a, own_tokens, 1, 1)
    for i in range(1, R):
        down_copy(i, r).start()
    apad[...] = jnp.zeros_like(apad)
    bpad[...] = jnp.zeros_like(bpad)
    apad[0:rank_rows, :] = a
    bpad[0:rank_rows, :] = b_ref[...]
    if C > 2:
        signal_line(line_sem.at[0])

    far_chunk = jnp.where(z > C - 1 - z, 0, C - 1)
    late_first = far_chunk * S + S - L
    late_owner = late_first // block_units
    late_slot = late_first % block_units

    def weights_of(first, rows):
        position = first + lax.broadcasted_iota(jnp.int32, (rows, LANES), 0)
        weights = jnp.zeros((rows, LANES), f32)
        start_row = 0
        for i in range(lengths.shape[1]):
            length = lengths[0, i]
            end_row = start_row + length
            inverse = 1.0 / jnp.full((1, LANES), length, jnp.int32).astype(f32)
            weights = jnp.where((position >= start_row) & (position < end_row), inverse, weights)
            start_row = end_row
        return weights

    row_weight[...] = weights_of(r * block_rows, block_rows)
    late_weight[...] = weights_of(late_first * sub, L * sub)

    load_w.wait()

    gram = contract_product(a, a, 1, 1)
    for start, width in tiles:
        span = pl.ds(start, width)
        st_in[r, 0:rank_rows, span] = jnp.dot(
            a, wx[:, span], preferred_element_type=f32
        ) + jnp.dot(
            gram, b_ref[:, span].astype(f32),
            precision=highest_precision, preferred_element_type=f32,
        )
        st_in[r, rank_rows:rank_rows + 8, span] = jnp.zeros((8, width), f32)
    depth = 256

    def norm_step(i, carry):
        rows = pl.ds(pl.multiple_of(i * depth, depth), depth)
        for start, width in tiles:
            span = pl.ds(start, width)
            merged = wx[rows, span].astype(f32) + contract_product(apad[:, rows], bpad[:, span], 0, 0)
            st_in[r, rank_rows:rank_rows + 1, span] += jnp.sum(merged * merged, axis=0, keepdims=True)
        return carry

    lax.fori_loop(0, features // depth, norm_step, 0)

    partner = p * 2 + (1 - q)

    def stat_near():
        return remote(st_in.at[r], st_in.at[r], stsend.at[0], strecv.at[0], {"row": partner})

    def stat_far(i, piece):
        return remote(
            st_pair.at[piece], st_pair.at[piece], stsend.at[1], strecv.at[1],
            {"row": ((p + i) % pairs) * 2 + q},
        )

    stat_near().start()

    def pair_stats():
        remote(st_in.at[partner], st_in.at[partner], stsend.at[0], strecv.at[0], {"row": partner}).wait_recv()
        st_pair[p] = st_in[r] + st_in[partner]
        for i in range(1, pairs):
            stat_far(i, p).start()

    def greet():
        pl.semaphore_wait(line_sem.at[0], line_count)
        for i in range(1, C - 2):
            signal_line(line_sem.at[i])
            if i < C - 3:
                pl.semaphore_wait(line_sem.at[i], line_count)

    def spread_down():
        if C > 3:
            pl.semaphore_wait(line_sem.at[C - 3], line_count)
        settle(down_in.at[pl.ds(0, R - 1)], dn_recv, {"row": partner}).wait_recv()
        down = down_in[0]
        for i in range(1, R):
            down = down + down_in[i]
        down_all[z] = down.astype(bf16)
        loop(C, lambda i: spread_copy(i, z).start())

    near = jnp.minimum(z, C - 1 - z)

    def place(k):
        j = k - S
        both = j < 2 * near * S
        rest = j - 2 * near * S
        distance = jnp.where(both, j // (2 * S) + 1, near + 1 + rest // S)
        s = jnp.where(both, (j % (2 * S)) // 2, rest % S)
        leftward = jnp.where(both, j % 2 == 0, z > C - 1 - z)
        chunk = jnp.where(leftward, z - distance, z + distance)
        own = k < S
        return jnp.where(own, z, chunk), jnp.where(own, k, s)

    def unit_of(k):
        c, s = place(k)
        return c * S + s

    def pair_copy(u):
        slot = u // block_units // 2 * block_units + u % block_units
        return remote(sb.at[u], pin.at[u], ssend.at[u], precv.at[slot], {"row": p * 2 + (1 - q)})

    def far_copy(u, owner_pair):
        return remote(
            sb.at[u], xin.at[p, u % block_units], ssend.at[u],
            xrecv.at[(p - owner_pair + pairs) % pairs - 1, u % block_units],
            {"row": owner_pair * 2 + q},
        )

    late_pair, late_core = late_owner // 2, late_owner % 2

    def late_far(i):
        rows = pl.ds(pl.multiple_of(late_slot * sub, sub), L * sub)
        return remote(cot.at[rows], late_cot, late_send.at[i], late_recv, {"row": ((p + i) % pairs) * 2 + q})

    def late_near():
        return remote(late_cot, late_cot, late_send.at[0], late_recv, {"row": partner})

    def back_copy(i, piece):
        return remote(back_in.at[piece], back_in.at[piece], bk_send, bk_recv, {"row": (r + i) % R})

    def scale_copy(i, piece):
        return remote(scale_in.at[piece], scale_in.at[piece], sc_send, sc_recv, device1(i))

    def group_sum(g, me, device, src, box, out, s1, r1, s2, r2):
        width = max(LANES, src.shape[1] // g)
        pieces = src.shape[1] // width

        def part(j):
            return pl.ds(pl.multiple_of(j * width, width), width)

        def scatter(i):
            return remote(src.at[:, part((me + i) % g % pieces)], box.at[i], s1, r1, device(i))

        def spread(i, j):
            return remote(out.at[:, part(j % pieces)], out.at[:, part(j % pieces)], s2, r2, device(i))

        def await_pieces(count, sem, sent):
            if count > 0:
                copies = settle(box.at[pl.ds(0, count)], sem, device(1))
                copies.wait_send() if sent else copies.wait_recv()

        def await_owners(sem, sent):
            if pieces == g:
                await_pieces(pieces - 1, sem, sent)
            else:
                @pl.when(me < pieces)
                def _():
                    await_pieces(pieces - 1, sem, sent)

                @pl.when(me >= pieces)
                def _():
                    await_pieces(pieces, sem, sent)

        def begin():
            def send(i):
                @pl.when((me + i) % g < pieces)
                def _():
                    scatter(i).start()

            loop(g, send)

        def middle():
            @pl.when(me < pieces)
            def _():
                await_pieces(g - 1, r1, False)
                out[:, part(me % pieces)] = lax.fori_loop(
                    1, g, lambda i, total: total + box[i], src[:, part(me % pieces)]
                )
                loop(g, lambda i: spread(i, me).start())

        def end():
            await_owners(r2, False)

        def drain():
            await_owners(s1, True)

            @pl.when(me < pieces)
            def _():
                await_pieces(g - 1, s2, True)

        return begin, middle, end, drain

    begin1, middle1, end1, drain1 = group_sum(
        g1, me1, device1, bsum, box1, bsum_all, r1a, r1b, r1c, r1d
    )

    def early():
        if pairs > 1:
            settle(st_pair.at[pl.ds(0, pairs - 1)], strecv.at[1], {"row": partner}).wait_recv()
        stats = st_pair[0]
        for i in range(1, pairs):
            stats = stats + st_pair[i]
        merged_factor[...] = stats[0:rank_rows]
        norm = jnp.sqrt(stats[rank_rows:rank_rows + 1] + norm_eps)
        col_norm[...] = norm
        col_scale[...] = magnitude[...] / norm
        coefficient_scale[...] = -magnitude[...] / (norm * norm * norm)
        load_c.wait()
        scale_in[me1] = jnp.zeros((1, cols), f32)
        for v in range(block_units):
            rows = pl.ds(v * sub, sub)
            weight = row_weight[rows, 0:1]
            for start, width in tiles:
                span = pl.ds(start, width)
                grad_out = cot[rows, span].astype(f32) * weight
                pg[rows, span] = (grad_out * col_scale[:, span]).astype(bf16)
        back_in[r] = contract_product(b_ref[...], pg[...], 1, 1).astype(bf16)
        for i in range(1, R):
            back_copy(i, r).start()

    def middle():
        settle(down_all.at[pl.ds(0, C - 1)], dz_recv, {"row": partner}).wait_recv()
        for start, width in tiles:
            span = pl.ds(start, width)
            total = jnp.zeros((rank_rows, width), f32)
            for i in range(chunks):
                down = down_all[r * chunks + i]
                total = total + jnp.dot(
                    down, pg[i * S * sub:(i + 1) * S * sub, span], preferred_element_type=f32
                )
                acc[i * S:(i + 1) * S, :, span] = contract_product(
                    down, b_ref[:, span], 0, 0
                ).reshape(S, sub, width)
            bsum[:, span] = total
        if D > 1:
            pl.semaphore_wait(plane_sem, D - 1)
        begin1()

        @pl.when(r == late_owner)
        def _():
            for i in range(L):
                rows = pl.ds(pl.multiple_of((late_slot + i) * sub, sub), sub)
                weight = row_weight[rows, 0:1]
                for start, width in tiles:
                    span = pl.ds(start, width)
                    grad_out = cot[rows, span].astype(f32) * weight
                    scale_in[me1, :, span] += jnp.sum(
                        grad_out * acc[late_slot + i, :, span], axis=0, keepdims=True
                    )

    def send_late():
        @pl.when(r == late_owner)
        def _():
            for i in range(1, pairs):
                late_far(i).start()
            late_cot[...] = cot[pl.ds(pl.multiple_of(late_slot * sub, sub), L * sub), :]

    def pass_late():
        @pl.when(q == late_core)
        def _():
            @pl.when(p != late_pair)
            def _():
                late_near().wait_recv()

            late_near().start()

    def multiply(k):
        c, s = place(k)
        u = c * S + s
        owner = u // block_units

        @pl.when(k >= S)
        def _():
            hop(u, 0).wait_recv()

            @pl.when((c < z) & (z < C - 1))
            def _():
                hop(u, 1).start()

            @pl.when((c > z) & (z > 0))
            def _():
                hop(u, 0).start()

        slot = k % 2
        for start, width in tiles:
            span = pl.ds(start, width)
            pb[slot, :, span] = jnp.dot(gath[u], wx[:, span], preferred_element_type=f32)

        @pl.when(k >= units - L)
        def _():
            @pl.when((k == units - L) & (q != late_core))
            def _():
                late_near().wait_recv()

            rows = pl.ds(pl.multiple_of((k - units + L) * sub, sub), sub)
            weight = late_weight[rows, 0:1]
            for start, width in tiles:
                span = pl.ds(start, width)
                grad_out = late_cot[rows, span].astype(f32) * weight
                scale_in[me1, :, span] += jnp.sum(grad_out * pb[slot, :, span], axis=0, keepdims=True)

        @pl.when(k == units - 1)
        def _():
            loop(g1, lambda i: scale_copy(i, me1).start())

        @pl.when(owner % 2 != q)
        def _():
            sb[u] = pb[slot].astype(bf16)
            pair_copy(u).start()

    def combine(k):
        u = unit_of(k)
        owner = u // block_units
        slot = k % 2

        @pl.when(owner % 2 == q)
        def _():
            pair_copy(u).wait_recv()
            total = pb[slot] + pin[u].astype(f32)

            @pl.when(owner // 2 == p)
            def _():
                own_sum[u % block_units] = total

            @pl.when(owner // 2 != p)
            def _():
                sb[u] = total.astype(bf16)
                far_copy(u, owner // 2).start()

    def factor_term(k):
        u = unit_of(k)
        block = u // block_units
        rows = pl.ds(pl.multiple_of((u % block_units) * sub, sub), sub)
        back = back_rows[block, rows, :]
        for start, width in feature_tiles:
            span = pl.ds(start, width)
            fsum[:, span] += contract_product(back, gath[u, :, span], 0, 0)[0:rank_rows]

    def finish(k):
        u = unit_of(k)

        @pl.when(u // block_units == r)
        def _():
            v = u % block_units
            for i in range(1, pairs):
                other = (p + i) % pairs
                remote(
                    sb.at[v], xin.at[other, v], ssend.at[v], xrecv.at[i - 1, v], {"row": other * 2 + q}
                ).wait_recv()
            rows = pl.ds(pl.multiple_of(v * sub, sub), sub)
            weight = row_weight[rows, 0:1]
            for start, width in tiles:
                span = pl.ds(start, width)
                query = acc[v, :, span] + own_sum[v, :, span]
                for i in range(1, pairs):
                    query = query + xin[(p + i) % pairs, v, :, span].astype(f32)
                projected[rows, span] = (query * col_scale[:, span]).astype(bf16)
                grad_out = cot[rows, span].astype(f32) * weight

                @pl.when(k < units - L)
                def _():
                    scale_in[me1, :, span] += jnp.sum(grad_out * query, axis=0, keepdims=True)

    def each(first, last, body):
        def turn(i, carry):
            body(i)
            return carry

        lax.fori_loop(first, last, turn, 0)

    fsum[...] = jnp.zeros_like(fsum)

    def step(k, carry):
        @pl.when(k > 0)
        def _():
            combine(k - 1)

        @pl.when(k == 1)
        def _():
            pair_stats()

        if C > 2:
            @pl.when(k == 2)
            def _():
                greet()

        @pl.when(k == S)
        def _():
            spread_down()

        @pl.when(k == half)
        def _():
            early()

        @pl.when(k == half + 1)
        def _():
            send_late()

        @pl.when(k == half + 2)
        def _():
            middle()

        @pl.when(k == catch_up)
        def _():
            settle(back_in.at[pl.ds(0, R - 1)], bk_recv, {"row": partner}).wait_recv()
            one = (
                lax.broadcasted_iota(jnp.int32, (rank_rows, LANES), 0)
                == lax.broadcasted_iota(jnp.int32, (rank_rows, LANES), 1)
            ).astype(f32).astype(bf16)
            for j in range(R):
                back_rows[j] = contract_product(back_in[j], one, 0, 0).astype(bf16)

        @pl.when(k >= catch_up)
        def _():
            done = rate * (k - catch_up)
            each(jnp.minimum(done, k - 1), jnp.minimum(done + rate, k), factor_term)
            each(jnp.minimum(done, k - 2), jnp.minimum(done + rate, k - 1), finish)

        @pl.when(k == catch_up + 1)
        def _():
            pass_late()

        @pl.when(k == units - 2)
        def _():
            middle1()

        multiply(k)
        return carry

    lax.fori_loop(0, units, step, 0)

    factor_term(units - 1)

    def group_copy(i, piece):
        return remote(fsum_in.at[piece], fsum_in.at[piece], fs_send, fs_recv, {"dp": (d + i) % D})

    fsum_in[d] = fsum[...].astype(bf16)
    for i in range(1, D):
        group_copy(i, d).start()
    combine(units - 1)

    ends = (z == 0) | (z == C - 1)
    side = jnp.where(z == 0, 0, 1)

    def end_copy(i, t):
        target = jnp.where(z == 0, i, C - 1 - i)
        return remote(end_out.at[t], end_in.at[side, t], end_send.at[i], end_recv.at[side], {"col": target})

    def end_arrived(j):
        settle(end_in.at[j], end_recv.at[j], {"row": partner}).wait_recv()
        for t, (start, width) in enumerate(feature_tiles):
            message[:, pl.ds(start, width)] += end_in[j, t].astype(f32)

    def line_copy(direction):
        target = z - 1 if direction == 0 else z + 1
        return remote(
            line_out.at[direction], line_in.at[direction], ln_send.at[direction], ln_recv.at[direction],
            {"col": target},
        )

    settle(scale_in.at[pl.ds(0, g1 - 1)], sc_recv, device1(1)).wait_recv()
    scale_grad = scale_in[0]
    for j in range(1, g1):
        scale_grad = scale_grad + scale_in[j]
    coefficient = scale_grad * coefficient_scale[...]
    scaled = (b_ref[...].astype(f32) * coefficient).astype(bf16)
    cross = contract_product(scaled, b_ref[...], 1, 1)
    for t, (start, width) in enumerate(feature_tiles):
        span = pl.ds(start, width)
        total = contract_product(scaled, wx[span, :], 1, 1) + jnp.dot(
            cross, a_ref[:, span].astype(f32),
            precision=highest_precision, preferred_element_type=f32,
        )
        total = total + fsum[:, span]
        if t == 0 and D > 1:
            settle(fsum_in.at[pl.ds(0, D - 1)], fs_recv, {"row": partner}).wait_recv()
        for i in range(1, D):
            total = total + fsum_in[(d - i + D) % D, :, span].astype(f32)
        message[:, span] = total

        @pl.when(ends)
        def _():
            end_out[t] = message[:, span].astype(bf16)
            for i in range(C - 1, 1, -1):
                end_copy(i, t).start()

    @pl.when(ends)
    def _():
        for t in range(len(feature_tiles)):
            end_copy(1, t).start()

    if C > 2:
        @pl.when((z > 0) & (z < C - 1))
        def _():
            own = message[...]
            for direction in (0, 1):
                more = (z < C - 2) if direction == 0 else (z > 1)

                @pl.when(more)
                def _():
                    line_copy(direction).wait_recv()
                    incoming = line_in[direction].astype(f32)
                    line_out[direction] = (own + incoming).astype(bf16)
                    message[...] += incoming

                @pl.when(jnp.logical_not(more))
                def _():
                    line_out[direction] = own.astype(bf16)

                line_copy(direction).start()

    each(units - 2, units, finish)
    grad_mag[...] = scale_grad / col_norm[...]
    end1()
    grad_b[...] = bsum_all[...] + merged_factor[...] * coefficient

    drain1()
    settle(scale_in.at[pl.ds(0, g1 - 1)], sc_send, device1(1)).wait_send()
    settle(back_in.at[pl.ds(0, R - 1)], bk_send, {"row": partner}).wait_send()
    settle(down_in.at[pl.ds(0, R - 1)], dn_send, {"row": partner}).wait_send()
    settle(down_all.at[pl.ds(0, C - 1)], dz_send, {"row": partner}).wait_send()
    if D > 1:
        settle(fsum_in.at[pl.ds(0, D - 1)], fs_send, {"row": partner}).wait_send()

    stat_near().wait_send()
    if pairs > 1:
        settle(st_pair.at[pl.ds(0, pairs - 1)], stsend.at[1], {"row": partner}).wait_send()

    @pl.when(r == late_owner)
    def _():
        for i in range(1, pairs):
            late_far(i).wait_send()

    @pl.when(q == late_core)
    def _():
        late_near().wait_send()

    def drain(u, carry):
        c = u // S
        owner = u // block_units

        @pl.when((owner % 2 != q) | (owner // 2 != p))
        def _():
            pair_copy(u).wait_send()

        @pl.when((c <= z) & (z < C - 1))
        def _():
            hop(u, 1).wait_send()

        @pl.when((c >= z) & (z > 0))
        def _():
            hop(u, 0).wait_send()

        return carry

    lax.fori_loop(0, units, drain, 0)

    if C > 2:
        @pl.when(z == 0)
        def _():
            line_copy(0).wait_recv()
            message[...] += line_in[0].astype(f32)

        @pl.when(z == C - 1)
        def _():
            line_copy(1).wait_recv()
            message[...] += line_in[1].astype(f32)

    @pl.when(z > 0)
    def _():
        end_arrived(0)

    @pl.when(z < C - 1)
    def _():
        end_arrived(1)

    factor_grad[...] = message[...]

    @pl.when(ends)
    def _():
        for i in range(C - 1, 0, -1):
            settle(end_out, end_send.at[i], {"row": partner}).wait_send()

    if C > 2:
        @pl.when((z > 0) & (z < C - 1))
        def _():
            line_copy(0).wait_send()
            line_copy(1).wait_send()


def hand_over_kernel(*refs):
    n = (len(refs) - 1) // 2
    sources, targets, sems = refs[:n], refs[n:2 * n], refs[-1]
    stores = [pltpu.make_async_copy(sources[i], targets[i], sems.at[i]) for i in range(n)]
    for store in stores:
        store.start()
    for store in stores:
        store.wait()


def per_device(
    tokens,
    frozen_weight,
    input_adapter_factor,
    output_adapter_factor,
    magnitude,
    cotangent,
    sequence_lengths,
):
    D, C, R = lax.axis_size("dp"), lax.axis_size("col"), lax.axis_size("row")
    local_rows, features = tokens.shape
    block_rows, cols = cotangent.shape
    rank_rows = input_adapter_factor.shape[0]
    S, L = 4, 2
    feature_tiles = features // FEATURE_TILE
    sub = local_rows // S
    units = C * S
    block_units = units // R
    g1 = D * R
    vmem = pl.BlockSpec(memory_space=pltpu.VMEM)
    hbm = pl.BlockSpec(memory_space=pl.ANY)
    dma = pltpu.SemaphoreType.DMA
    regular = pltpu.SemaphoreType.REGULAR
    f32, bf16 = jnp.float32, jnp.bfloat16
    results = pl.pallas_call(
        functools.partial(adapter_kernel, D, C, R, S, L),
        out_shape=(
            pltpu.VMEM((block_rows, cols), bf16),
            pltpu.VMEM((1, cols), f32),
            pltpu.VMEM((rank_rows, features), f32),
            pltpu.VMEM((rank_rows, cols), f32),
        ),
        in_specs=[hbm] * 7,
        out_specs=(vmem, vmem, vmem, vmem),
        scratch_shapes=[
            pltpu.SMEM(sequence_lengths.shape, jnp.int32),
            pltpu.VMEM((features, cols), bf16),
            pltpu.VMEM((units, sub, features), bf16),
            pltpu.VMEM((units, sub, cols), bf16),
            pltpu.VMEM((units, sub, cols), bf16),
            pltpu.VMEM((R // 2, block_units, sub, cols), bf16),
            pltpu.VMEM((2, sub, cols), f32),
            pltpu.VMEM((R, rank_rows + 8, cols), f32),
            pltpu.VMEM((R // 2, rank_rows + 8, cols), f32),
            pltpu.VMEM((rank_rows, features), bf16),
            pltpu.VMEM((rank_rows, cols), bf16),
            pltpu.VMEM((1, cols), f32),
            pltpu.VMEM((LANES, features), bf16),
            pltpu.VMEM((LANES, cols), bf16),
            pltpu.VMEM((block_units, sub, cols), f32),
            pltpu.VMEM((block_units, sub, cols), f32),
            pltpu.VMEM((block_rows, cols), bf16),
            pltpu.VMEM((block_rows, cols), bf16),
            pltpu.VMEM((L * sub, cols), bf16),
            pltpu.VMEM((block_rows, LANES), f32),
            pltpu.VMEM((L * sub, LANES), f32),
            pltpu.VMEM((R, rank_rows, local_rows), f32),
            pltpu.VMEM((C, rank_rows, local_rows), bf16),
            pltpu.VMEM((rank_rows, cols), f32),
            pltpu.VMEM((1, cols), f32),
            pltpu.VMEM((1, cols), f32),
            pltpu.VMEM((1, cols), f32),
            pltpu.VMEM((g1, 1, cols), f32),
            pltpu.VMEM((R, rank_rows, block_rows), bf16),
            pltpu.VMEM((R, block_rows, LANES), bf16),
            pltpu.VMEM((rank_rows, cols), f32),
            pltpu.VMEM((rank_rows, cols), f32),
            pltpu.VMEM((g1, rank_rows, max(LANES, cols // g1)), f32),
            pltpu.VMEM((rank_rows, features), f32),
            pltpu.VMEM((D, rank_rows, features), bf16),
            pltpu.VMEM((rank_rows, features), f32),
            pltpu.VMEM((2, rank_rows, features), bf16),
            pltpu.VMEM((2, rank_rows, features), bf16),
            pltpu.VMEM((feature_tiles, rank_rows, features // feature_tiles), bf16),
            pltpu.VMEM((2, feature_tiles, rank_rows, features // feature_tiles), bf16),
            dma((6,)),
            dma((S,)),
            regular,
            pltpu.SemaphoreType.REGULAR((max(1, C - 2),)),
            dma((units + S,)),
            dma((units,)),
            dma((units,)),
            dma((R // 2 * block_units,)),
            dma((max(1, R // 2 - 1), block_units)),
            dma((2,)),
            dma((2,)),
            dma(()),
            dma(()),
            dma(()),
            dma(()),
            dma((R // 2,)),
            dma(()),
            dma(()),
            dma(()),
            dma(()),
            dma(()),
            dma(()),
            dma(()),
            dma((2,)),
            dma((2,)),
            dma((C,)),
            dma((2,)),
        ] + [dma(())] * 4,
        compiler_params=pltpu.CompilerParams(
            collective_id=0, has_side_effects=True, vmem_limit_bytes=VMEM_LIMIT
        ),
    )(
        tokens.reshape(S, sub, features), frozen_weight, input_adapter_factor,
        output_adapter_factor, magnitude.reshape(1, cols), cotangent, sequence_lengths,
    )
    results = [pltpu.with_memory_space_constraint(x, pltpu.VMEM) for x in results]
    projected, grad_mag, factor_grad, grad_b = pl.pallas_call(
        hand_over_kernel,
        out_shape=tuple(jax.ShapeDtypeStruct(x.shape, x.dtype) for x in results),
        in_specs=[vmem] * len(results),
        out_specs=(hbm,) * len(results),
        scratch_shapes=[dma((len(results),))],
    )(*results)
    return projected, grad_mag.reshape(cols), factor_grad, grad_b


def solution(mesh):
    in_specs = (
        P(("dp", "col"), "row"),
        P("row", "col"),
        P(None, "row"),
        P(None, "col"),
        P("col"),
        P(("dp", "row"), "col"),
        P("dp", None),
    )
    out_specs = (P(("dp", "row"), "col"), P("col"), P(None, "row"), P(None, "col"))
    return jax.shard_map(
        per_device, mesh=mesh, in_specs=in_specs, out_specs=out_specs, check_vma=False
    )
```

```python
import functools

import jax
import jax.numpy as jnp
from jax import lax
from jax.experimental import pallas as pl
from jax.experimental.pallas import tpu as pltpu
from jax.sharding import PartitionSpec as P

norm_eps = 1e-06
highest_precision = lax.Precision.HIGHEST
MESH = pl.DeviceIdType.MESH
LANES = 128
FEATURE_TILE = 512
TURN = 256
PIECES = 4
VMEM_LIMIT = 56 * 1024 * 1024


def contract_product(left, right, left_dim, right_dim):
    return lax.dot_general(
        left, right, (((left_dim,), (right_dim,)), ((), ())), preferred_element_type=jnp.float32
    )


def column_tiles(width, tile):
    return [(start, min(tile, width - start)) for start in range(0, width, tile)]


def adapter_kernel(
    D, C, R, S, L,
    tok, w_hbm, a_hbm, b_hbm, magnitude_hbm, cot_hbm, lengths_hbm,
    projected, grad_mag, factor_grad, grad_b,
    lengths, wx, wt, gath, sb, pin, xin, pb, st_in, st_pair, a_ref, b_ref, magnitude, apad, bpad, acc, own_sum, pg, cot, late_cot,
    row_weight, late_weight, down_in, down_all, merged_factor, col_norm, col_scale, coefficient_scale,
    scale_in, back_in, back_rows, bsum, bsum_all, box1, fsum, fsum_in, message, line_in, line_out, end_out, end_in,
    load_sem, tok_sem, plane_sem, line_sem, gsend, grecv, qsend, qrecv, ssend, precv, xrecv, stsend, strecv,
    dn_send, dn_recv, dz_send, dz_recv, late_send, late_recv, sc_send, sc_recv, bk_send, bk_recv,
    fs_send, fs_recv, ln_send, ln_recv, end_send, end_recv, r1a, r1b, r1c, r1d,
):
    z = lax.axis_index("col")
    r = lax.axis_index("row")
    d = lax.axis_index("dp")
    p, q = r // 2, r % 2
    pairs = R // 2
    sub, features = tok.shape[1], tok.shape[2]
    cols = w_hbm.shape[1]
    rank_rows = a_ref.shape[0]
    units = C * S
    block_units = units // R
    block_rows = block_units * sub
    chunks = block_units // S
    tiles = column_tiles(cols, 512)
    feature_tiles = column_tiles(features, FEATURE_TILE)
    f32, bf16 = jnp.float32, jnp.bfloat16
    half = units // 2
    catch_up = half + 3
    rate = 4

    g1 = D * R
    me1 = d * R + r

    def device1(i):
        peer = (me1 + i) % g1
        return {"dp": peer // R, "row": peer % R}

    def loop(n, body):
        def turn(i, carry):
            body(i)
            return carry

        lax.fori_loop(1, n, turn, 0)

    def remote(src, dst, send_sem, recv_sem, device):
        return pltpu.make_async_remote_copy(
            src_ref=src, dst_ref=dst, send_sem=send_sem, recv_sem=recv_sem,
            device_id=device, device_id_type=MESH,
        )

    def settle(view, sem, device):
        return remote(view, view, sem, sem, device)

    def signal(sem, device):
        pl.semaphore_signal(sem, inc=1, device_id=device, device_id_type=MESH)

    def signal_line(sem):
        @pl.when(z > 0)
        def _():
            signal(sem, {"col": z - 1})

        @pl.when(z < C - 1)
        def _():
            signal(sem, {"col": z + 1})

    line_count = jnp.where(z > 0, 1, 0) + jnp.where(z < C - 1, 1, 0)

    barrier = pltpu.get_barrier_semaphore()
    signal_line(barrier)
    for i in range(1, R):
        signal(barrier, {"row": (r + i) % R})
    for i in range(1, D):
        signal(barrier, {"dp": (d + i) % D})

    def load_tok(s):
        return pltpu.make_async_copy(tok.at[s], gath.at[z * S + s], tok_sem.at[s])

    small_loads = [
        pltpu.make_async_copy(a_hbm, a_ref, load_sem.at[0]),
        pltpu.make_async_copy(b_hbm, b_ref, load_sem.at[1]),
        pltpu.make_async_copy(magnitude_hbm, magnitude, load_sem.at[2]),
        pltpu.make_async_copy(lengths_hbm, lengths, load_sem.at[5]),
    ]
    load_w = pltpu.make_async_copy(w_hbm, wx, load_sem.at[3])
    load_c = pltpu.make_async_copy(cot_hbm, cot, load_sem.at[4])
    for s in range(S):
        load_tok(s).start()
    for load in small_loads:
        load.start()
    load_w.start()
    load_c.start()

    pl.semaphore_wait(barrier, line_count + R - 1 + D - 1)

    def hop(u, direction):
        target = z - 1 if direction == 0 else z + 1
        return remote(gath.at[u], gath.at[u], gsend.at[direction], grecv.at[u], {"col": target})

    ends = (z == 0) | (z == C - 1)
    piece = features // PIECES

    def hop_piece(u, j):
        view = gath.at[u, :, pl.ds(j * piece, piece)]
        origin = jnp.where(u // S == 0, 0, 1)
        target = jnp.clip(jnp.where(u // S == 0, z + 1, z - 1), 0, C - 1)
        return remote(view, view, qsend.at[origin], qrecv.at[origin, j], {"col": target})

    for s in range(S):
        load_tok(s).wait()
        whole = jnp.logical_not(ends) if s == S - 1 else True

        @pl.when((z > 0) & whole)
        def _():
            hop(z * S + s, 0).start()

        @pl.when((z < C - 1) & whole)
        def _():
            hop(z * S + s, 1).start()

    @pl.when(ends)
    def _():
        for j in range(PIECES):
            hop_piece(z * S + S - 1, j).start()

    for i in range(1, D):
        signal(plane_sem, {"dp": (d + i) % D})
    for load in small_loads:
        load.wait()

    def down_copy(i, piece):
        return remote(
            down_in.at[piece], down_in.at[piece], dn_send, dn_recv, {"row": (r + i) % R}
        )

    def spread_copy(i, piece):
        return remote(
            down_all.at[piece], down_all.at[piece], dz_send, dz_recv, {"col": (z + i) % C}
        )

    a = a_ref[...]
    own_tokens = gath[pl.ds(z * S, S)].reshape(S * sub, features)
    down_in[r] = contract_product(a, own_tokens, 1, 1)
    for i in range(1, R):
        down_copy(i, r).start()
    apad[...] = jnp.zeros_like(apad)
    bpad[...] = jnp.zeros_like(bpad)
    apad[0:rank_rows, :] = a
    bpad[0:rank_rows, :] = b_ref[...]
    if C > 2:
        signal_line(line_sem.at[0])

    far_chunk = jnp.where(z > C - 1 - z, 0, C - 1)
    late_first = far_chunk * S + S - L
    late_owner = late_first // block_units
    late_slot = late_first % block_units

    def weights_of(first, rows):
        position = first + lax.broadcasted_iota(jnp.int32, (rows, LANES), 0)
        weights = jnp.zeros((rows, LANES), f32)
        start_row = 0
        for i in range(lengths.shape[1]):
            length = lengths[0, i]
            end_row = start_row + length
            inverse = 1.0 / jnp.full((1, LANES), length, jnp.int32).astype(f32)
            weights = jnp.where((position >= start_row) & (position < end_row), inverse, weights)
            start_row = end_row
        return weights

    row_weight[...] = weights_of(r * block_rows, block_rows)
    late_weight[...] = weights_of(late_first * sub, L * sub)

    load_w.wait()

    gram = contract_product(a, a, 1, 1)
    for start, width in tiles:
        span = pl.ds(start, width)
        st_in[r, 0:rank_rows, span] = jnp.dot(
            a, wx[:, span], preferred_element_type=f32
        ) + jnp.dot(
            gram, b_ref[:, span].astype(f32),
            precision=highest_precision, preferred_element_type=f32,
        )
        st_in[r, rank_rows:rank_rows + 8, span] = jnp.zeros((8, width), f32)
    depth = 256

    def norm_step(i, carry):
        rows = pl.ds(pl.multiple_of(i * depth, depth), depth)
        for start, width in tiles:
            span = pl.ds(start, width)
            merged = wx[rows, span].astype(f32) + contract_product(apad[:, rows], bpad[:, span], 0, 0)
            st_in[r, rank_rows:rank_rows + 1, span] += jnp.sum(merged * merged, axis=0, keepdims=True)
        return carry

    lax.fori_loop(0, features // depth, norm_step, 0)

    partner = p * 2 + (1 - q)

    def stat_near():
        return remote(st_in.at[r], st_in.at[r], stsend.at[0], strecv.at[0], {"row": partner})

    def stat_far(i, piece):
        return remote(
            st_pair.at[piece], st_pair.at[piece], stsend.at[1], strecv.at[1],
            {"row": ((p + i) % pairs) * 2 + q},
        )

    stat_near().start()

    def pair_stats():
        remote(st_in.at[partner], st_in.at[partner], stsend.at[0], strecv.at[0], {"row": partner}).wait_recv()
        st_pair[p] = st_in[r] + st_in[partner]
        for i in range(1, pairs):
            stat_far(i, p).start()

    def greet():
        pl.semaphore_wait(line_sem.at[0], line_count)
        for i in range(1, C - 2):
            signal_line(line_sem.at[i])
            if i < C - 3:
                pl.semaphore_wait(line_sem.at[i], line_count)

    def spread_down():
        if C > 3:
            pl.semaphore_wait(line_sem.at[C - 3], line_count)
        settle(down_in.at[pl.ds(0, R - 1)], dn_recv, {"row": partner}).wait_recv()
        down = down_in[0]
        for i in range(1, R):
            down = down + down_in[i]
        down_all[z] = down.astype(bf16)
        @pl.when(r == z * S // block_units)
        def _():
            loop(C, lambda i: spread_copy(i, z).start())

    near = jnp.minimum(z, C - 1 - z)

    def place(k):
        j = k - S
        both = j < 2 * near * S
        rest = j - 2 * near * S
        distance = jnp.where(both, j // (2 * S) + 1, near + 1 + rest // S)
        s = jnp.where(both, (j % (2 * S)) // 2, rest % S)
        leftward = jnp.where(both, j % 2 == 0, z > C - 1 - z)
        chunk = jnp.where(leftward, z - distance, z + distance)
        own = k < S
        return jnp.where(own, z, chunk), jnp.where(own, k, s)

    def unit_of(k):
        c, s = place(k)
        return c * S + s

    def pair_copy(u):
        slot = u // block_units // 2 * block_units + u % block_units
        return remote(sb.at[u], pin.at[u], ssend.at[0], precv.at[slot], {"row": p * 2 + (1 - q)})

    def far_copy(u, owner_pair):
        return remote(
            sb.at[u], xin.at[p, u % block_units], ssend.at[1],
            xrecv.at[(p - owner_pair + pairs) % pairs - 1, u % block_units],
            {"row": owner_pair * 2 + q},
        )

    late_pair, late_core = late_owner // 2, late_owner % 2

    def late_far(i):
        rows = pl.ds(pl.multiple_of(late_slot * sub, sub), L * sub)
        return remote(cot.at[rows], late_cot, late_send.at[i], late_recv, {"row": ((p + i) % pairs) * 2 + q})

    def late_near():
        return remote(late_cot, late_cot, late_send.at[0], late_recv, {"row": partner})

    def back_copy(i, piece):
        return remote(back_in.at[piece], back_in.at[piece], bk_send, bk_recv, {"row": (r + i) % R})

    def scale_copy(i, piece):
        return remote(scale_in.at[piece], scale_in.at[piece], sc_send, sc_recv, device1(i))

    def group_sum(g, me, device, src, box, out, s1, r1, s2, r2):
        width = max(LANES, src.shape[1] // g)
        pieces = src.shape[1] // width

        def part(j):
            return pl.ds(pl.multiple_of(j * width, width), width)

        def scatter(i):
            return remote(src.at[:, part((me + i) % g % pieces)], box.at[i], s1, r1, device(i))

        def spread(i, j):
            return remote(out.at[:, part(j % pieces)], out.at[:, part(j % pieces)], s2, r2, device(i))

        def await_pieces(count, sem, sent):
            if count > 0:
                copies = settle(box.at[pl.ds(0, count)], sem, device(1))
                copies.wait_send() if sent else copies.wait_recv()

        def await_owners(sem, sent):
            if pieces == g:
                await_pieces(pieces - 1, sem, sent)
            else:
                @pl.when(me < pieces)
                def _():
                    await_pieces(pieces - 1, sem, sent)

                @pl.when(me >= pieces)
                def _():
                    await_pieces(pieces, sem, sent)

        def begin():
            def send(i):
                @pl.when((me + i) % g < pieces)
                def _():
                    scatter(i).start()

            loop(g, send)

        def middle():
            @pl.when(me < pieces)
            def _():
                await_pieces(g - 1, r1, False)
                out[:, part(me % pieces)] = lax.fori_loop(
                    1, g, lambda i, total: total + box[i], src[:, part(me % pieces)]
                )
                loop(g, lambda i: spread(i, me).start())

        def end():
            await_owners(r2, False)

        def drain():
            await_owners(s1, True)

            @pl.when(me < pieces)
            def _():
                await_pieces(g - 1, s2, True)

        return begin, middle, end, drain

    begin1, middle1, end1, drain1 = group_sum(
        g1, me1, device1, bsum, box1, bsum_all, r1a, r1b, r1c, r1d
    )

    def early():
        if pairs > 1:
            settle(st_pair.at[pl.ds(0, pairs - 1)], strecv.at[1], {"row": partner}).wait_recv()
        stats = st_pair[0]
        for i in range(1, pairs):
            stats = stats + st_pair[i]
        merged_factor[...] = stats[0:rank_rows]
        norm = jnp.sqrt(stats[rank_rows:rank_rows + 1] + norm_eps)
        col_norm[...] = norm
        col_scale[...] = magnitude[...] / norm
        coefficient_scale[...] = -magnitude[...] / (norm * norm * norm)
        load_c.wait()
        scale_in[me1] = jnp.zeros((1, cols), f32)
        for v in range(block_units):
            rows = pl.ds(v * sub, sub)
            weight = row_weight[rows, 0:1]
            for start, width in tiles:
                span = pl.ds(start, width)
                grad_out = cot[rows, span].astype(f32) * weight
                pg[rows, span] = (grad_out * col_scale[:, span]).astype(bf16)
        back_in[r] = contract_product(b_ref[...], pg[...], 1, 1).astype(bf16)
        for i in range(1, R):
            back_copy(i, r).start()

    def middle():
        @pl.when(z // chunks != r)
        def _():
            settle(down_all.at[pl.ds(0, chunks)], dz_recv, {"row": partner}).wait_recv()

        if chunks > 1:
            @pl.when(z // chunks == r)
            def _():
                settle(down_all.at[pl.ds(0, chunks - 1)], dz_recv, {"row": partner}).wait_recv()

        for start, width in tiles:
            span = pl.ds(start, width)
            total = jnp.zeros((rank_rows, width), f32)
            for i in range(chunks):
                down = down_all[r * chunks + i]
                total = total + jnp.dot(
                    down, pg[i * S * sub:(i + 1) * S * sub, span], preferred_element_type=f32
                )
                acc[i * S:(i + 1) * S, :, span] = contract_product(
                    down, b_ref[:, span], 0, 0
                ).reshape(S, sub, width)
            bsum[:, span] = total
        if D > 1:
            pl.semaphore_wait(plane_sem, D - 1)
        begin1()

        @pl.when(r == late_owner)
        def _():
            for i in range(L):
                rows = pl.ds(pl.multiple_of((late_slot + i) * sub, sub), sub)
                weight = row_weight[rows, 0:1]
                for start, width in tiles:
                    span = pl.ds(start, width)
                    grad_out = cot[rows, span].astype(f32) * weight
                    scale_in[me1, :, span] += jnp.sum(
                        grad_out * acc[late_slot + i, :, span], axis=0, keepdims=True
                    )

    def send_late():
        @pl.when(r == late_owner)
        def _():
            for i in range(1, pairs):
                late_far(i).start()
            late_cot[...] = cot[pl.ds(pl.multiple_of(late_slot * sub, sub), L * sub), :]

    def pass_late():
        @pl.when(q == late_core)
        def _():
            @pl.when(p != late_pair)
            def _():
                late_near().wait_recv()

            late_near().start()

    def multiply(k):
        c, s = place(k)
        u = c * S + s
        owner = u // block_units

        split = (k >= S) & (s == S - 1) & ((c == 0) | (c == C - 1))

        @pl.when((k >= S) & jnp.logical_not(split))
        def _():
            hop(u, 0).wait_recv()

            @pl.when((c < z) & (z < C - 1))
            def _():
                hop(u, 1).start()

            @pl.when((c > z) & (z > 0))
            def _():
                hop(u, 0).start()

        slot = k % 2

        @pl.when(jnp.logical_not(split))
        def _():
            for start, width in tiles:
                span = pl.ds(start, width)
                pb[slot, :, span] = jnp.dot(gath[u], wx[:, span], preferred_element_type=f32)

        @pl.when(split)
        def _():
            for j in range(PIECES):
                hop_piece(u, j).wait_recv()

                @pl.when(((c == 0) & (z < C - 1)) | ((c != 0) & (z > 0)))
                def _():
                    hop_piece(u, j).start()

                part = pl.ds(j * piece, piece)
                for start, width in tiles:
                    span = pl.ds(start, width)
                    product = jnp.dot(gath[u, :, part], wx[part, span], preferred_element_type=f32)
                    pb[slot, :, span] = product if j == 0 else pb[slot, :, span] + product

        @pl.when(k >= units - L)
        def _():
            @pl.when((k == units - L) & (q != late_core))
            def _():
                late_near().wait_recv()

            rows = pl.ds(pl.multiple_of((k - units + L) * sub, sub), sub)
            weight = late_weight[rows, 0:1]
            for start, width in tiles:
                span = pl.ds(start, width)
                grad_out = late_cot[rows, span].astype(f32) * weight
                scale_in[me1, :, span] += jnp.sum(grad_out * pb[slot, :, span], axis=0, keepdims=True)

        @pl.when(k == units - 1)
        def _():
            loop(g1, lambda i: scale_copy(i, me1).start())

        @pl.when(owner % 2 != q)
        def _():
            sb[u] = pb[slot].astype(bf16)
            pair_copy(u).start()

    def combine(k):
        u = unit_of(k)
        owner = u // block_units
        slot = k % 2

        @pl.when(owner % 2 == q)
        def _():
            pair_copy(u).wait_recv()
            total = pb[slot] + pin[u].astype(f32)

            @pl.when(owner // 2 == p)
            def _():
                own_sum[u % block_units] = total

            @pl.when(owner // 2 != p)
            def _():
                sb[u] = total.astype(bf16)
                far_copy(u, owner // 2).start()

    def factor_term(k):
        u = unit_of(k)
        block = u // block_units
        rows = pl.ds(pl.multiple_of((u % block_units) * sub, sub), sub)
        back = back_rows[block, rows, :]
        for start, width in feature_tiles:
            span = pl.ds(start, width)
            fsum[:, span] += contract_product(back, gath[u, :, span], 0, 0)[0:rank_rows]

    def finish(k):
        u = unit_of(k)

        @pl.when(u // block_units == r)
        def _():
            v = u % block_units
            for i in range(1, pairs):
                other = (p + i) % pairs
                remote(
                    sb.at[v], xin.at[other, v], ssend.at[1], xrecv.at[i - 1, v], {"row": other * 2 + q}
                ).wait_recv()
            rows = pl.ds(pl.multiple_of(v * sub, sub), sub)
            weight = row_weight[rows, 0:1]
            for start, width in tiles:
                span = pl.ds(start, width)
                query = acc[v, :, span] + own_sum[v, :, span]
                for i in range(1, pairs):
                    query = query + xin[(p + i) % pairs, v, :, span].astype(f32)
                projected[rows, span] = (query * col_scale[:, span]).astype(bf16)
                grad_out = cot[rows, span].astype(f32) * weight

                @pl.when(k < units - L)
                def _():
                    scale_in[me1, :, span] += jnp.sum(grad_out * query, axis=0, keepdims=True)

    def each(first, last, body):
        def turn(i, carry):
            body(i)
            return carry

        lax.fori_loop(first, last, turn, 0)

    fsum[...] = jnp.zeros_like(fsum)

    def step(k, carry):
        @pl.when(k > 0)
        def _():
            combine(k - 1)

        @pl.when(k == 1)
        def _():
            pair_stats()

        turned = k - (units - 1 - features // TURN)

        @pl.when(ends & (turned >= 0) & (turned < features // TURN))
        def _():
            per_tile = FEATURE_TILE // TURN
            rows = pl.ds(pl.multiple_of(turned * TURN, TURN), TURN)
            lanes = pl.ds(pl.multiple_of(turned % per_tile * TURN, TURN), TURN)
            wt[turned // per_tile, :, lanes] = wx[rows, :].T

        if C > 2:
            @pl.when(k == 2)
            def _():
                greet()

        @pl.when(k == S)
        def _():
            spread_down()

        @pl.when(k == half)
        def _():
            early()

        @pl.when(k == half + 1)
        def _():
            send_late()

        @pl.when(k == half + 2)
        def _():
            middle()

        @pl.when(k == catch_up)
        def _():
            settle(back_in.at[pl.ds(0, R - 1)], bk_recv, {"row": partner}).wait_recv()
            one = (
                lax.broadcasted_iota(jnp.int32, (rank_rows, LANES), 0)
                == lax.broadcasted_iota(jnp.int32, (rank_rows, LANES), 1)
            ).astype(f32).astype(bf16)
            for j in range(R):
                back_rows[j] = contract_product(back_in[j], one, 0, 0).astype(bf16)

        @pl.when(k >= catch_up)
        def _():
            done = rate * (k - catch_up)
            each(jnp.minimum(done, k - 1), jnp.minimum(done + rate, k), factor_term)
            each(jnp.minimum(done, k - 2), jnp.minimum(done + rate, k - 1), finish)

        @pl.when(k == catch_up + 1)
        def _():
            pass_late()

        @pl.when(k == units - 2)
        def _():
            middle1()

        multiply(k)
        return carry

    lax.fori_loop(0, units, step, 0)

    factor_term(units - 1)

    def group_copy(i, piece):
        return remote(fsum_in.at[piece], fsum_in.at[piece], fs_send, fs_recv, {"dp": (d + i) % D})

    fsum_in[d] = fsum[...].astype(bf16)
    for i in range(1, D):
        group_copy(i, d).start()
    combine(units - 1)

    side = jnp.where(z == 0, 0, 1)

    def end_copy(i, t):
        target = jnp.where(z == 0, i, C - 1 - i)
        return remote(end_out.at[t], end_in.at[side, t], end_send.at[i], end_recv.at[side], {"col": target})

    def end_arrived(j):
        settle(end_in.at[j], end_recv.at[j], {"row": partner}).wait_recv()
        for t, (start, width) in enumerate(feature_tiles):
            message[:, pl.ds(start, width)] += end_in[j, t].astype(f32)

    def line_copy(direction):
        target = z - 1 if direction == 0 else z + 1
        return remote(
            line_out.at[direction], line_in.at[direction], ln_send.at[direction], ln_recv.at[direction],
            {"col": target},
        )

    settle(scale_in.at[pl.ds(0, g1 - 1)], sc_recv, device1(1)).wait_recv()
    scale_grad = scale_in[0]
    for j in range(1, g1):
        scale_grad = scale_grad + scale_in[j]
    coefficient = scale_grad * coefficient_scale[...]
    scaled = (b_ref[...].astype(f32) * coefficient).astype(bf16)
    cross = contract_product(scaled, b_ref[...], 1, 1)
    if D > 1:
        settle(fsum_in.at[pl.ds(0, D - 1)], fs_recv, {"row": partner}).wait_recv()

    def term(t, product):
        start, width = feature_tiles[t]
        span = pl.ds(start, width)
        total = product + jnp.dot(
            cross, a_ref[:, span].astype(f32),
            precision=highest_precision, preferred_element_type=f32,
        )
        total = total + fsum[:, span]
        for i in range(1, D):
            total = total + fsum_in[(d - i + D) % D, :, span].astype(f32)
        message[:, span] = total
        return total

    @pl.when(ends)
    def _():
        for t in range(len(feature_tiles)):
            end_out[t] = term(t, jnp.dot(scaled, wt[t], preferred_element_type=f32)).astype(bf16)
            end_copy(C - 1, t).start()
        for i in range(C - 2, 0, -1):
            for t in range(len(feature_tiles)):
                end_copy(i, t).start()

    @pl.when(jnp.logical_not(ends))
    def _():
        for t, (start, width) in enumerate(feature_tiles):
            term(t, contract_product(scaled, wx[pl.ds(start, width), :], 1, 1))

    if C > 2:
        @pl.when((z > 0) & (z < C - 1))
        def _():
            own = message[...]
            for direction in (0, 1):
                more = (z < C - 2) if direction == 0 else (z > 1)

                @pl.when(more)
                def _():
                    line_copy(direction).wait_recv()
                    incoming = line_in[direction].astype(f32)
                    line_out[direction] = (own + incoming).astype(bf16)
                    message[...] += incoming

                @pl.when(jnp.logical_not(more))
                def _():
                    line_out[direction] = own.astype(bf16)

                line_copy(direction).start()

    each(units - 2, units, finish)
    grad_mag[...] = scale_grad / col_norm[...]
    end1()
    grad_b[...] = bsum_all[...] + merged_factor[...] * coefficient

    drain1()
    settle(scale_in.at[pl.ds(0, g1 - 1)], sc_send, device1(1)).wait_send()
    settle(back_in.at[pl.ds(0, R - 1)], bk_send, {"row": partner}).wait_send()
    settle(down_in.at[pl.ds(0, R - 1)], dn_send, {"row": partner}).wait_send()

    @pl.when(r == z * S // block_units)
    def _():
        settle(down_all.at[pl.ds(0, C - 1)], dz_send, {"row": partner}).wait_send()

    if D > 1:
        settle(fsum_in.at[pl.ds(0, D - 1)], fs_send, {"row": partner}).wait_send()

    stat_near().wait_send()
    if pairs > 1:
        settle(st_pair.at[pl.ds(0, pairs - 1)], stsend.at[1], {"row": partner}).wait_send()

    @pl.when(r == late_owner)
    def _():
        for i in range(1, pairs):
            late_far(i).wait_send()

    @pl.when(q == late_core)
    def _():
        late_near().wait_send()

    settle(sb.at[pl.ds(0, units // 2)], ssend.at[0], {"row": partner}).wait_send()
    if pairs > 1:
        settle(sb.at[pl.ds(0, block_units * (pairs - 1))], ssend.at[1], {"row": partner}).wait_send()
    for i in range(C):
        @pl.when(z == i)
        def _():
            if i > 0:
                settle(gath.at[pl.ds(0, (C - i) * S - 1)], gsend.at[0], {"row": partner}).wait_send()
                settle(gath.at[0], qsend.at[1], {"row": partner}).wait_send()
            if i < C - 1:
                settle(gath.at[pl.ds(0, (i + 1) * S - 1)], gsend.at[1], {"row": partner}).wait_send()
                settle(gath.at[0], qsend.at[0], {"row": partner}).wait_send()

    if C > 2:
        @pl.when(z == 0)
        def _():
            line_copy(0).wait_recv()
            message[...] += line_in[0].astype(f32)

        @pl.when(z == C - 1)
        def _():
            line_copy(1).wait_recv()
            message[...] += line_in[1].astype(f32)

    @pl.when(z > 0)
    def _():
        end_arrived(0)

    @pl.when(z < C - 1)
    def _():
        end_arrived(1)

    factor_grad[...] = message[...]

    @pl.when(ends)
    def _():
        for i in range(C - 1, 0, -1):
            settle(end_out, end_send.at[i], {"row": partner}).wait_send()

    if C > 2:
        @pl.when((z > 0) & (z < C - 1))
        def _():
            line_copy(0).wait_send()
            line_copy(1).wait_send()


def hand_over_kernel(*refs):
    n = (len(refs) - 1) // 2
    sources, targets, sems = refs[:n], refs[n:2 * n], refs[-1]
    stores = [pltpu.make_async_copy(sources[i], targets[i], sems.at[i]) for i in range(n)]
    for store in stores:
        store.start()
    for store in stores:
        store.wait()


def per_device(
    tokens,
    frozen_weight,
    input_adapter_factor,
    output_adapter_factor,
    magnitude,
    cotangent,
    sequence_lengths,
):
    D, C, R = lax.axis_size("dp"), lax.axis_size("col"), lax.axis_size("row")
    local_rows, features = tokens.shape
    block_rows, cols = cotangent.shape
    rank_rows = input_adapter_factor.shape[0]
    S, L = 4, 2
    feature_tiles = features // FEATURE_TILE
    sub = local_rows // S
    units = C * S
    block_units = units // R
    g1 = D * R
    vmem = pl.BlockSpec(memory_space=pltpu.VMEM)
    hbm = pl.BlockSpec(memory_space=pl.ANY)
    dma = pltpu.SemaphoreType.DMA
    regular = pltpu.SemaphoreType.REGULAR
    f32, bf16 = jnp.float32, jnp.bfloat16
    results = pl.pallas_call(
        functools.partial(adapter_kernel, D, C, R, S, L),
        out_shape=(
            pltpu.VMEM((block_rows, cols), bf16),
            pltpu.VMEM((1, cols), f32),
            pltpu.VMEM((rank_rows, features), f32),
            pltpu.VMEM((rank_rows, cols), f32),
        ),
        in_specs=[hbm] * 7,
        out_specs=(vmem, vmem, vmem, vmem),
        scratch_shapes=[
            pltpu.SMEM(sequence_lengths.shape, jnp.int32),
            pltpu.VMEM((features, cols), bf16),
            pltpu.VMEM((feature_tiles, cols, features // feature_tiles), bf16),
            pltpu.VMEM((units, sub, features), bf16),
            pltpu.VMEM((units, sub, cols), bf16),
            pltpu.VMEM((units, sub, cols), bf16),
            pltpu.VMEM((R // 2, block_units, sub, cols), bf16),
            pltpu.VMEM((2, sub, cols), f32),
            pltpu.VMEM((R, rank_rows + 8, cols), f32),
            pltpu.VMEM((R // 2, rank_rows + 8, cols), f32),
            pltpu.VMEM((rank_rows, features), bf16),
            pltpu.VMEM((rank_rows, cols), bf16),
            pltpu.VMEM((1, cols), f32),
            pltpu.VMEM((LANES, features), bf16),
            pltpu.VMEM((LANES, cols), bf16),
            pltpu.VMEM((block_units, sub, cols), f32),
            pltpu.VMEM((block_units, sub, cols), f32),
            pltpu.VMEM((block_rows, cols), bf16),
            pltpu.VMEM((block_rows, cols), bf16),
            pltpu.VMEM((L * sub, cols), bf16),
            pltpu.VMEM((block_rows, LANES), f32),
            pltpu.VMEM((L * sub, LANES), f32),
            pltpu.VMEM((R, rank_rows, local_rows), f32),
            pltpu.VMEM((C, rank_rows, local_rows), bf16),
            pltpu.VMEM((rank_rows, cols), f32),
            pltpu.VMEM((1, cols), f32),
            pltpu.VMEM((1, cols), f32),
            pltpu.VMEM((1, cols), f32),
            pltpu.VMEM((g1, 1, cols), f32),
            pltpu.VMEM((R, rank_rows, block_rows), bf16),
            pltpu.VMEM((R, block_rows, LANES), bf16),
            pltpu.VMEM((rank_rows, cols), f32),
            pltpu.VMEM((rank_rows, cols), f32),
            pltpu.VMEM((g1, rank_rows, max(LANES, cols // g1)), f32),
            pltpu.VMEM((rank_rows, features), f32),
            pltpu.VMEM((D, rank_rows, features), bf16),
            pltpu.VMEM((rank_rows, features), f32),
            pltpu.VMEM((2, rank_rows, features), bf16),
            pltpu.VMEM((2, rank_rows, features), bf16),
            pltpu.VMEM((feature_tiles, rank_rows, features // feature_tiles), bf16),
            pltpu.VMEM((2, feature_tiles, rank_rows, features // feature_tiles), bf16),
            dma((6,)),
            dma((S,)),
            regular,
            pltpu.SemaphoreType.REGULAR((max(1, C - 2),)),
            dma((2,)),
            dma((units,)),
            dma((2,)),
            dma((2, PIECES)),
            dma((2,)),
            dma((R // 2 * block_units,)),
            dma((max(1, R // 2 - 1), block_units)),
            dma((2,)),
            dma((2,)),
            dma(()),
            dma(()),
            dma(()),
            dma(()),
            dma((R // 2,)),
            dma(()),
            dma(()),
            dma(()),
            dma(()),
            dma(()),
            dma(()),
            dma(()),
            dma((2,)),
            dma((2,)),
            dma((C,)),
            dma((2,)),
        ] + [dma(())] * 4,
        compiler_params=pltpu.CompilerParams(
            collective_id=0, has_side_effects=True, vmem_limit_bytes=VMEM_LIMIT
        ),
    )(
        tokens.reshape(S, sub, features), frozen_weight, input_adapter_factor,
        output_adapter_factor, magnitude.reshape(1, cols), cotangent, sequence_lengths,
    )
    results = [pltpu.with_memory_space_constraint(x, pltpu.VMEM) for x in results]
    projected, grad_mag, factor_grad, grad_b = pl.pallas_call(
        hand_over_kernel,
        out_shape=tuple(jax.ShapeDtypeStruct(x.shape, x.dtype) for x in results),
        in_specs=[vmem] * len(results),
        out_specs=(hbm,) * len(results),
        scratch_shapes=[dma((len(results),))],
    )(*results)
    return projected, grad_mag.reshape(cols), factor_grad, grad_b


def solution(mesh):
    in_specs = (
        P(("dp", "col"), "row"),
        P("row", "col"),
        P(None, "row"),
        P(None, "col"),
        P("col"),
        P(("dp", "row"), "col"),
        P("dp", None),
    )
    out_specs = (P(("dp", "row"), "col"), P("col"), P(None, "row"), P(None, "col"))
    return jax.shard_map(
        per_device, mesh=mesh, in_specs=in_specs, out_specs=out_specs, check_vma=False
    )
```

```python
import functools

import jax
import jax.numpy as jnp
from jax import lax
from jax.experimental import pallas as pl
from jax.experimental.pallas import tpu as pltpu
from jax.sharding import PartitionSpec as P

norm_eps = 1e-06
highest_precision = lax.Precision.HIGHEST
MESH = pl.DeviceIdType.MESH
LANES = 128
FEATURE_TILE = 512
TURN = 256
PIECES = 8
VMEM_LIMIT = 56 * 1024 * 1024


def contract_product(left, right, left_dim, right_dim):
    return lax.dot_general(
        left, right, (((left_dim,), (right_dim,)), ((), ())), preferred_element_type=jnp.float32
    )


def column_tiles(width, tile):
    return [(start, min(tile, width - start)) for start in range(0, width, tile)]


def adapter_kernel(
    D, C, R, S, L,
    tok, w_hbm, a_hbm, b_hbm, magnitude_hbm, cot_hbm, lengths_hbm,
    projected, grad_mag, factor_grad, grad_b,
    lengths, wx, wt, gath, sb, pin, xin, pb, st_in, st_pair, a_ref, b_ref, magnitude, apad, bpad, acc, own_sum, pg, cot, late_cot,
    row_weight, late_weight, down_in, down_all, merged_factor, col_norm, col_scale, coefficient_scale,
    scale_in, back_in, back_rows, back_far, bsum, bsum_all, box1, fsum, fsum_in, message, line_in, line_out, end_out, end_in, cross_out, cross_in,
    load_sem, tok_sem, plane_sem, line_sem, gsend, grecv, qsend, qrecv, ssend, precv, xrecv, stsend, strecv,
    dn_send, dn_recv, dz_send, dz_recv, late_send, late_recv, sc_send, sc_recv, bk_send, bk_recv,
    fs_send, fs_recv, ln_send, ln_recv, end_send, end_recv, bf_send, bf_recv, cx_send, cx_recv, r1a, r1b, r1c, r1d,
):
    z = lax.axis_index("col")
    r = lax.axis_index("row")
    d = lax.axis_index("dp")
    p, q = r // 2, r % 2
    pairs = R // 2
    sub, features = tok.shape[1], tok.shape[2]
    cols = w_hbm.shape[1]
    rank_rows = a_ref.shape[0]
    units = C * S
    block_units = units // R
    block_rows = block_units * sub
    chunks = block_units // S
    tiles = column_tiles(cols, 512)
    feature_tiles = column_tiles(features, FEATURE_TILE)
    f32, bf16 = jnp.float32, jnp.bfloat16
    half = units // 2
    catch_up = half + 3
    rate = 4

    g1 = D * R
    me1 = d * R + r

    def device1(i):
        peer = (me1 + i) % g1
        return {"dp": peer // R, "row": peer % R}

    def loop(n, body):
        def turn(i, carry):
            body(i)
            return carry

        lax.fori_loop(1, n, turn, 0)

    def remote(src, dst, send_sem, recv_sem, device):
        return pltpu.make_async_remote_copy(
            src_ref=src, dst_ref=dst, send_sem=send_sem, recv_sem=recv_sem,
            device_id=device, device_id_type=MESH,
        )

    def settle(view, sem, device):
        return remote(view, view, sem, sem, device)

    def signal(sem, device):
        pl.semaphore_signal(sem, inc=1, device_id=device, device_id_type=MESH)

    def signal_line(sem):
        @pl.when(z > 0)
        def _():
            signal(sem, {"col": z - 1})

        @pl.when(z < C - 1)
        def _():
            signal(sem, {"col": z + 1})

    line_count = jnp.where(z > 0, 1, 0) + jnp.where(z < C - 1, 1, 0)

    barrier = pltpu.get_barrier_semaphore()
    signal_line(barrier)
    for i in range(1, R):
        signal(barrier, {"row": (r + i) % R})
    for i in range(1, D):
        signal(barrier, {"dp": (d + i) % D})

    def load_tok(s):
        return pltpu.make_async_copy(tok.at[s], gath.at[z * S + s], tok_sem.at[s])

    small_loads = [
        pltpu.make_async_copy(a_hbm, a_ref, load_sem.at[0]),
        pltpu.make_async_copy(b_hbm, b_ref, load_sem.at[1]),
        pltpu.make_async_copy(magnitude_hbm, magnitude, load_sem.at[2]),
        pltpu.make_async_copy(lengths_hbm, lengths, load_sem.at[5]),
    ]
    load_w = pltpu.make_async_copy(w_hbm, wx, load_sem.at[3])
    load_c = pltpu.make_async_copy(cot_hbm, cot, load_sem.at[4])
    for s in range(S):
        load_tok(s).start()
    for load in small_loads:
        load.start()
    load_w.start()
    load_c.start()

    pl.semaphore_wait(barrier, line_count + R - 1 + D - 1)

    def hop(u, direction):
        target = z - 1 if direction == 0 else z + 1
        return remote(gath.at[u], gath.at[u], gsend.at[direction], grecv.at[u], {"col": target})

    ends = (z == 0) | (z == C - 1)
    piece = features // PIECES

    def hop_piece(u, j):
        view = gath.at[u, :, pl.ds(j * piece, piece)]
        origin = jnp.where(u // S == 0, 0, 1)
        target = jnp.clip(jnp.where(u // S == 0, z + 1, z - 1), 0, C - 1)
        return remote(view, view, qsend.at[origin], qrecv.at[origin, j], {"col": target})

    for s in range(S):
        load_tok(s).wait()
        whole = jnp.logical_not(ends) if s == S - 1 else True

        @pl.when((z > 0) & whole)
        def _():
            hop(z * S + s, 0).start()

        @pl.when((z < C - 1) & whole)
        def _():
            hop(z * S + s, 1).start()

    @pl.when(ends)
    def _():
        for j in range(PIECES):
            hop_piece(z * S + S - 1, j).start()

    for i in range(1, D):
        signal(plane_sem, {"dp": (d + i) % D})
    for load in small_loads:
        load.wait()

    def down_copy(i, piece):
        return remote(
            down_in.at[piece], down_in.at[piece], dn_send, dn_recv, {"row": (r + i) % R}
        )

    def spread_copy(i, piece):
        return remote(
            down_all.at[piece], down_all.at[piece], dz_send, dz_recv, {"col": (z + i) % C}
        )

    a = a_ref[...]
    own_tokens = gath[pl.ds(z * S, S)].reshape(S * sub, features)
    down_in[r] = contract_product(a, own_tokens, 1, 1)
    for i in range(1, R):
        down_copy(i, r).start()
    apad[...] = jnp.zeros_like(apad)
    bpad[...] = jnp.zeros_like(bpad)
    apad[0:rank_rows, :] = a
    bpad[0:rank_rows, :] = b_ref[...]
    if C > 2:
        signal_line(line_sem.at[0])

    far_chunk = jnp.where(z > C - 1 - z, 0, C - 1)
    late_first = far_chunk * S + S - L
    late_owner = late_first // block_units
    late_slot = late_first % block_units

    def weights_of(first, rows):
        position = first + lax.broadcasted_iota(jnp.int32, (rows, LANES), 0)
        weights = jnp.zeros((rows, LANES), f32)
        start_row = 0
        for i in range(lengths.shape[1]):
            length = lengths[0, i]
            end_row = start_row + length
            inverse = 1.0 / jnp.full((1, LANES), length, jnp.int32).astype(f32)
            weights = jnp.where((position >= start_row) & (position < end_row), inverse, weights)
            start_row = end_row
        return weights

    row_weight[...] = weights_of(r * block_rows, block_rows)
    late_weight[...] = weights_of(late_first * sub, L * sub)

    load_w.wait()

    gram = contract_product(a, a, 1, 1)
    for start, width in tiles:
        span = pl.ds(start, width)
        st_in[r, 0:rank_rows, span] = jnp.dot(
            a, wx[:, span], preferred_element_type=f32
        ) + jnp.dot(
            gram, b_ref[:, span].astype(f32),
            precision=highest_precision, preferred_element_type=f32,
        )
        st_in[r, rank_rows:rank_rows + 8, span] = jnp.zeros((8, width), f32)
    depth = 256

    def norm_step(i, carry):
        rows = pl.ds(pl.multiple_of(i * depth, depth), depth)
        for start, width in tiles:
            span = pl.ds(start, width)
            merged = wx[rows, span].astype(f32) + contract_product(apad[:, rows], bpad[:, span], 0, 0)
            st_in[r, rank_rows:rank_rows + 1, span] += jnp.sum(merged * merged, axis=0, keepdims=True)
        return carry

    lax.fori_loop(0, features // depth, norm_step, 0)

    partner = p * 2 + (1 - q)

    def stat_near():
        return remote(st_in.at[r], st_in.at[r], stsend.at[0], strecv.at[0], {"row": partner})

    def stat_far(i, piece):
        return remote(
            st_pair.at[piece], st_pair.at[piece], stsend.at[1], strecv.at[1],
            {"row": ((p + i) % pairs) * 2 + q},
        )

    stat_near().start()

    def pair_stats():
        remote(st_in.at[partner], st_in.at[partner], stsend.at[0], strecv.at[0], {"row": partner}).wait_recv()
        st_pair[p] = st_in[r] + st_in[partner]
        for i in range(1, pairs):
            stat_far(i, p).start()

    def greet():
        pl.semaphore_wait(line_sem.at[0], line_count)
        for i in range(1, C - 2):
            signal_line(line_sem.at[i])
            if i < C - 3:
                pl.semaphore_wait(line_sem.at[i], line_count)

    def spread_down():
        if C > 3:
            pl.semaphore_wait(line_sem.at[C - 3], line_count)
        settle(down_in.at[pl.ds(0, R - 1)], dn_recv, {"row": partner}).wait_recv()
        down = down_in[0]
        for i in range(1, R):
            down = down + down_in[i]
        down_all[z] = down.astype(bf16)
        @pl.when(r == z * S // block_units)
        def _():
            loop(C, lambda i: spread_copy(i, z).start())

    near = jnp.minimum(z, C - 1 - z)

    def place(k):
        j = k - S
        both = j < 2 * near * S
        rest = j - 2 * near * S
        distance = jnp.where(both, j // (2 * S) + 1, near + 1 + rest // S)
        s = jnp.where(both, (j % (2 * S)) // 2, rest % S)
        leftward = jnp.where(both, j % 2 == 0, z > C - 1 - z)
        chunk = jnp.where(leftward, z - distance, z + distance)
        own = k < S
        return jnp.where(own, z, chunk), jnp.where(own, k, s)

    def unit_of(k):
        c, s = place(k)
        return c * S + s

    def pair_copy(u):
        slot = u // block_units // 2 * block_units + u % block_units
        return remote(sb.at[u], pin.at[u], ssend.at[0], precv.at[slot], {"row": p * 2 + (1 - q)})

    def far_copy(u, owner_pair):
        return remote(
            sb.at[u], xin.at[p, u % block_units], ssend.at[1],
            xrecv.at[(p - owner_pair + pairs) % pairs - 1, u % block_units],
            {"row": owner_pair * 2 + q},
        )

    late_pair, late_core = late_owner // 2, late_owner % 2

    def late_far(i):
        rows = pl.ds(pl.multiple_of(late_slot * sub, sub), L * sub)
        return remote(cot.at[rows], late_cot, late_send.at[i], late_recv, {"row": ((p + i) % pairs) * 2 + q})

    def late_near():
        return remote(late_cot, late_cot, late_send.at[0], late_recv, {"row": partner})

    def back_copy(i, piece):
        return remote(back_in.at[piece], back_in.at[piece], bk_send, bk_recv, {"row": (r + i) % R})

    def far_back_copy():
        unit = far_chunk * S + S - 1
        rows = pl.ds(pl.multiple_of(unit % block_units * sub, sub), sub)
        return remote(back_rows.at[unit // block_units, rows, :], back_far, bf_send, bf_recv, {"col": C - 1 - z})

    def scale_copy(i, piece):
        return remote(scale_in.at[piece], scale_in.at[piece], sc_send, sc_recv, device1(i))

    def group_sum(g, me, device, src, box, out, s1, r1, s2, r2):
        width = max(LANES, src.shape[1] // g)
        pieces = src.shape[1] // width

        def part(j):
            return pl.ds(pl.multiple_of(j * width, width), width)

        def scatter(i):
            return remote(src.at[:, part((me + i) % g % pieces)], box.at[i], s1, r1, device(i))

        def spread(i, j):
            return remote(out.at[:, part(j % pieces)], out.at[:, part(j % pieces)], s2, r2, device(i))

        def await_pieces(count, sem, sent):
            if count > 0:
                copies = settle(box.at[pl.ds(0, count)], sem, device(1))
                copies.wait_send() if sent else copies.wait_recv()

        def await_owners(sem, sent):
            if pieces == g:
                await_pieces(pieces - 1, sem, sent)
            else:
                @pl.when(me < pieces)
                def _():
                    await_pieces(pieces - 1, sem, sent)

                @pl.when(me >= pieces)
                def _():
                    await_pieces(pieces, sem, sent)

        def begin():
            def send(i):
                @pl.when((me + i) % g < pieces)
                def _():
                    scatter(i).start()

            loop(g, send)

        def middle():
            @pl.when(me < pieces)
            def _():
                await_pieces(g - 1, r1, False)
                out[:, part(me % pieces)] = lax.fori_loop(
                    1, g, lambda i, total: total + box[i], src[:, part(me % pieces)]
                )
                loop(g, lambda i: spread(i, me).start())

        def end():
            await_owners(r2, False)

        def drain():
            await_owners(s1, True)

            @pl.when(me < pieces)
            def _():
                await_pieces(g - 1, s2, True)

        return begin, middle, end, drain

    begin1, middle1, end1, drain1 = group_sum(
        g1, me1, device1, bsum, box1, bsum_all, r1a, r1b, r1c, r1d
    )

    def early():
        if pairs > 1:
            settle(st_pair.at[pl.ds(0, pairs - 1)], strecv.at[1], {"row": partner}).wait_recv()
        stats = st_pair[0]
        for i in range(1, pairs):
            stats = stats + st_pair[i]
        merged_factor[...] = stats[0:rank_rows]
        norm = jnp.sqrt(stats[rank_rows:rank_rows + 1] + norm_eps)
        col_norm[...] = norm
        col_scale[...] = magnitude[...] / norm
        coefficient_scale[...] = -magnitude[...] / (norm * norm * norm)
        load_c.wait()
        scale_in[me1] = jnp.zeros((1, cols), f32)
        for v in range(block_units):
            rows = pl.ds(v * sub, sub)
            weight = row_weight[rows, 0:1]
            for start, width in tiles:
                span = pl.ds(start, width)
                grad_out = cot[rows, span].astype(f32) * weight
                pg[rows, span] = (grad_out * col_scale[:, span]).astype(bf16)
        back_in[r] = contract_product(b_ref[...], pg[...], 1, 1).astype(bf16)
        for i in range(1, R):
            back_copy(i, r).start()

    def middle():
        @pl.when(z // chunks != r)
        def _():
            settle(down_all.at[pl.ds(0, chunks)], dz_recv, {"row": partner}).wait_recv()

        if chunks > 1:
            @pl.when(z // chunks == r)
            def _():
                settle(down_all.at[pl.ds(0, chunks - 1)], dz_recv, {"row": partner}).wait_recv()

        for start, width in tiles:
            span = pl.ds(start, width)
            total = jnp.zeros((rank_rows, width), f32)
            for i in range(chunks):
                down = down_all[r * chunks + i]
                total = total + jnp.dot(
                    down, pg[i * S * sub:(i + 1) * S * sub, span], preferred_element_type=f32
                )
                acc[i * S:(i + 1) * S, :, span] = contract_product(
                    down, b_ref[:, span], 0, 0
                ).reshape(S, sub, width)
            bsum[:, span] = total
        if D > 1:
            pl.semaphore_wait(plane_sem, D - 1)
        begin1()

        @pl.when(r == late_owner)
        def _():
            for i in range(L):
                rows = pl.ds(pl.multiple_of((late_slot + i) * sub, sub), sub)
                weight = row_weight[rows, 0:1]
                for start, width in tiles:
                    span = pl.ds(start, width)
                    grad_out = cot[rows, span].astype(f32) * weight
                    scale_in[me1, :, span] += jnp.sum(
                        grad_out * acc[late_slot + i, :, span], axis=0, keepdims=True
                    )

    def send_late():
        @pl.when(r == late_owner)
        def _():
            for i in range(1, pairs):
                late_far(i).start()
            late_cot[...] = cot[pl.ds(pl.multiple_of(late_slot * sub, sub), L * sub), :]

    def pass_late():
        @pl.when(q == late_core)
        def _():
            @pl.when(p != late_pair)
            def _():
                late_near().wait_recv()

            late_near().start()

    def multiply(k):
        c, s = place(k)
        u = c * S + s
        owner = u // block_units

        split = (k >= S) & (s == S - 1) & ((c == 0) | (c == C - 1))

        @pl.when((k >= S) & jnp.logical_not(split))
        def _():
            hop(u, 0).wait_recv()

            @pl.when((c < z) & (z < C - 1))
            def _():
                hop(u, 1).start()

            @pl.when((c > z) & (z > 0))
            def _():
                hop(u, 0).start()

        slot = k % 2

        @pl.when(jnp.logical_not(split))
        def _():
            for start, width in tiles:
                span = pl.ds(start, width)
                pb[slot, :, span] = jnp.dot(gath[u], wx[:, span], preferred_element_type=f32)

        @pl.when(split)
        def _():
            for j in range(PIECES):
                hop_piece(u, j).wait_recv()

                @pl.when(((c == 0) & (z < C - 1)) | ((c != 0) & (z > 0)))
                def _():
                    hop_piece(u, j).start()

                part = pl.ds(j * piece, piece)
                for start, width in tiles:
                    span = pl.ds(start, width)
                    product = jnp.dot(gath[u, :, part], wx[part, span], preferred_element_type=f32)
                    pb[slot, :, span] = product if j == 0 else pb[slot, :, span] + product

        @pl.when(k >= units - L)
        def _():
            @pl.when((k == units - L) & (q != late_core))
            def _():
                late_near().wait_recv()

            rows = pl.ds(pl.multiple_of((k - units + L) * sub, sub), sub)
            weight = late_weight[rows, 0:1]
            for start, width in tiles:
                span = pl.ds(start, width)
                grad_out = late_cot[rows, span].astype(f32) * weight
                scale_in[me1, :, span] += jnp.sum(grad_out * pb[slot, :, span], axis=0, keepdims=True)

        @pl.when(k == units - 1)
        def _():
            loop(g1, lambda i: scale_copy(i, me1).start())

        @pl.when(owner % 2 != q)
        def _():
            sb[u] = pb[slot].astype(bf16)
            pair_copy(u).start()

    def combine(k):
        u = unit_of(k)
        owner = u // block_units
        slot = k % 2

        @pl.when(owner % 2 == q)
        def _():
            pair_copy(u).wait_recv()
            total = pb[slot] + pin[u].astype(f32)

            @pl.when(owner // 2 == p)
            def _():
                own_sum[u % block_units] = total

            @pl.when(owner // 2 != p)
            def _():
                sb[u] = total.astype(bf16)
                far_copy(u, owner // 2).start()

    def factor_term(k):
        u = unit_of(k)
        block = u // block_units
        rows = pl.ds(pl.multiple_of((u % block_units) * sub, sub), sub)
        add_term(u, back_rows[block, rows, :])

    def add_term(u, back):
        for start, width in feature_tiles:
            span = pl.ds(start, width)
            fsum[:, span] += contract_product(back, gath[u, :, span], 0, 0)[0:rank_rows]

    def finish(k):
        u = unit_of(k)

        @pl.when(u // block_units == r)
        def _():
            v = u % block_units
            for i in range(1, pairs):
                other = (p + i) % pairs
                remote(
                    sb.at[v], xin.at[other, v], ssend.at[1], xrecv.at[i - 1, v], {"row": other * 2 + q}
                ).wait_recv()
            rows = pl.ds(pl.multiple_of(v * sub, sub), sub)
            weight = row_weight[rows, 0:1]
            for start, width in tiles:
                span = pl.ds(start, width)
                query = acc[v, :, span] + own_sum[v, :, span]
                for i in range(1, pairs):
                    query = query + xin[(p + i) % pairs, v, :, span].astype(f32)
                projected[rows, span] = (query * col_scale[:, span]).astype(bf16)
                grad_out = cot[rows, span].astype(f32) * weight

                @pl.when(k < units - L)
                def _():
                    scale_in[me1, :, span] += jnp.sum(grad_out * query, axis=0, keepdims=True)

    def each(first, last, body):
        def turn(i, carry):
            body(i)
            return carry

        lax.fori_loop(first, last, turn, 0)

    def group_copy(i, piece):
        return remote(fsum_in.at[piece], fsum_in.at[piece], fs_send, fs_recv, {"dp": (d + i) % D})

    def share_term():
        fsum_in[d] = fsum[...].astype(bf16)
        for i in range(1, D):
            group_copy(i, d).start()

    fsum[...] = jnp.zeros_like(fsum)
    cross_out[...] = jnp.zeros_like(cross_out)

    def step(k, carry):
        @pl.when(k > 0)
        def _():
            combine(k - 1)

        @pl.when(k == 1)
        def _():
            pair_stats()

        turned = k - (units - 1 - features // TURN)

        @pl.when(ends & (turned >= 0) & (turned < features // TURN))
        def _():
            per_tile = FEATURE_TILE // TURN
            rows = pl.ds(pl.multiple_of(turned * TURN, TURN), TURN)
            lanes = pl.ds(pl.multiple_of(turned % per_tile * TURN, TURN), TURN)
            wt[turned // per_tile, :, lanes] = wx[rows, :].T

        if C > 2:
            @pl.when(k == 2)
            def _():
                greet()

        @pl.when(k == S)
        def _():
            spread_down()

        @pl.when(k == half)
        def _():
            early()

        @pl.when(k == half + 1)
        def _():
            send_late()

        @pl.when(k == half + 2)
        def _():
            middle()

        @pl.when(k == catch_up)
        def _():
            settle(back_in.at[pl.ds(0, R - 1)], bk_recv, {"row": partner}).wait_recv()
            one = (
                lax.broadcasted_iota(jnp.int32, (rank_rows, LANES), 0)
                == lax.broadcasted_iota(jnp.int32, (rank_rows, LANES), 1)
            ).astype(f32).astype(bf16)
            for j in range(R):
                back_rows[j] = contract_product(back_in[j], one, 0, 0).astype(bf16)

            @pl.when(ends)
            def _():
                far_back_copy().start()

        @pl.when(k >= catch_up)
        def _():
            done = rate * (k - catch_up)
            each(jnp.minimum(done, k - 1), jnp.minimum(done + rate, k), factor_term)
            each(jnp.minimum(done, k - 2), jnp.minimum(done + rate, k - 1), finish)

        @pl.when((k == units - 2) & ends)
        def _():
            far_back_copy().wait_recv()
            add_term(z * S + S - 1, back_far[...])

        @pl.when((k == units - 1) & ends)
        def _():
            share_term()

        @pl.when(k == catch_up + 1)
        def _():
            pass_late()

        @pl.when(k == units - 2)
        def _():
            middle1()

        multiply(k)
        return carry

    lax.fori_loop(0, units, step, 0)

    @pl.when(jnp.logical_not(ends))
    def _():
        factor_term(units - 1)
        share_term()

    combine(units - 1)

    side = jnp.where(z == 0, 0, 1)

    def end_copy(i, t):
        target = jnp.where(z == 0, i, C - 1 - i)
        return remote(end_out.at[t], end_in.at[side, t], end_send.at[i], end_recv.at[side], {"col": target})

    def end_arrived(j):
        settle(end_in.at[j], end_recv.at[j], {"row": partner}).wait_recv()
        for t, (start, width) in enumerate(feature_tiles):
            message[:, pl.ds(start, width)] += end_in[j, t].astype(f32)

    def line_copy(direction):
        target = z - 1 if direction == 0 else z + 1
        return remote(
            line_out.at[direction], line_in.at[direction], ln_send.at[direction], ln_recv.at[direction],
            {"col": target},
        )

    settle(scale_in.at[pl.ds(0, g1 - 1)], sc_recv, device1(1)).wait_recv()
    scale_grad = scale_in[0]
    for j in range(1, g1):
        scale_grad = scale_grad + scale_in[j]
    coefficient = scale_grad * coefficient_scale[...]
    scaled = (b_ref[...].astype(f32) * coefficient).astype(bf16)
    if D > 1:
        settle(fsum_in.at[pl.ds(0, D - 1)], fs_recv, {"row": partner}).wait_recv()

    def term(t, product):
        start, width = feature_tiles[t]
        span = pl.ds(start, width)
        total = product + fsum[:, span]
        for i in range(1, D):
            total = total + fsum_in[(d - i + D) % D, :, span].astype(f32)
        message[:, span] = total
        return total

    def add_cross(cross):
        for start, width in feature_tiles:
            span = pl.ds(start, width)
            message[:, span] += jnp.dot(
                cross, a_ref[:, span].astype(f32),
                precision=highest_precision, preferred_element_type=f32,
            )

    def cross_copy(i):
        target = jnp.where(z == 0, i, C - 1 - i)
        return remote(cross_out, cross_in.at[side], cx_send, cx_recv.at[side], {"col": target})

    @pl.when(ends)
    def _():
        for t in range(len(feature_tiles)):
            end_out[t] = term(t, jnp.dot(scaled, wt[t], preferred_element_type=f32)).astype(bf16)
            end_copy(C - 1, t).start()
            if t == 0:
                cross_out[:, 0:rank_rows] = contract_product(scaled, b_ref[...], 1, 1)
                for i in range(C - 1, 0, -1):
                    cross_copy(i).start()
        for i in range(C - 2, 0, -1):
            for t in range(len(feature_tiles)):
                end_copy(i, t).start()

    @pl.when(jnp.logical_not(ends))
    def _():
        for t, (start, width) in enumerate(feature_tiles):
            term(t, contract_product(scaled, wx[pl.ds(start, width), :], 1, 1))
        add_cross(contract_product(scaled, b_ref[...], 1, 1))

    def drain_stream(direction):
        for i in range(C):
            count = (C - i) * S - 1 if direction == 0 else (i + 1) * S - 1
            if 0 <= i + 2 * direction - 1 < C:
                @pl.when(z == i)
                def _():
                    settle(gath.at[pl.ds(0, count)], gsend.at[direction], {"row": partner}).wait_send()
                    settle(gath.at[0], qsend.at[1 - direction], {"row": partner}).wait_send()

    if C > 2:
        @pl.when((z > 0) & (z < C - 1))
        def _():
            own = message[...]
            more = ((z < C - 2), (z > 1))
            for direction in (0, 1):
                @pl.when(jnp.logical_not(more[direction]))
                def _():
                    line_out[direction] = own.astype(bf16)
                    drain_stream(direction)
                    line_copy(direction).start()

            for direction in (0, 1):
                @pl.when(more[direction])
                def _():
                    line_copy(direction).wait_recv()
                    incoming = line_in[direction].astype(f32)
                    line_out[direction] = (own + incoming).astype(bf16)
                    message[...] += incoming
                    drain_stream(direction)
                    line_copy(direction).start()

    each(units - 2, units, finish)
    grad_mag[...] = scale_grad / col_norm[...]
    end1()
    grad_b[...] = bsum_all[...] + merged_factor[...] * coefficient

    drain1()
    settle(scale_in.at[pl.ds(0, g1 - 1)], sc_send, device1(1)).wait_send()
    settle(back_in.at[pl.ds(0, R - 1)], bk_send, {"row": partner}).wait_send()
    settle(down_in.at[pl.ds(0, R - 1)], dn_send, {"row": partner}).wait_send()

    @pl.when(r == z * S // block_units)
    def _():
        settle(down_all.at[pl.ds(0, C - 1)], dz_send, {"row": partner}).wait_send()

    if D > 1:
        settle(fsum_in.at[pl.ds(0, D - 1)], fs_send, {"row": partner}).wait_send()

    stat_near().wait_send()
    if pairs > 1:
        settle(st_pair.at[pl.ds(0, pairs - 1)], stsend.at[1], {"row": partner}).wait_send()

    @pl.when(r == late_owner)
    def _():
        for i in range(1, pairs):
            late_far(i).wait_send()

    @pl.when(q == late_core)
    def _():
        late_near().wait_send()

    settle(sb.at[pl.ds(0, units // 2)], ssend.at[0], {"row": partner}).wait_send()
    if pairs > 1:
        settle(sb.at[pl.ds(0, block_units * (pairs - 1))], ssend.at[1], {"row": partner}).wait_send()

    @pl.when(ends)
    def _():
        drain_stream(0)
        drain_stream(1)


    if C > 2:
        @pl.when(z == 0)
        def _():
            line_copy(0).wait_recv()
            message[...] += line_in[0].astype(f32)

        @pl.when(z == C - 1)
        def _():
            line_copy(1).wait_recv()
            message[...] += line_in[1].astype(f32)

    for j in (0, 1):
        @pl.when(z != j * (C - 1))
        def _():
            remote(cross_out, cross_in.at[j], cx_send, cx_recv.at[j], {"row": partner}).wait_recv()
            add_cross(cross_in[j, :, 0:rank_rows])

    @pl.when(ends)
    def _():
        add_cross(cross_out[:, 0:rank_rows])

    @pl.when(z > 0)
    def _():
        end_arrived(0)

    @pl.when(z < C - 1)
    def _():
        end_arrived(1)

    factor_grad[...] = message[...]

    @pl.when(ends)
    def _():
        far_back_copy().wait_send()
        settle(cross_in.at[pl.ds(0, C - 1)], cx_send, {"row": partner}).wait_send()
        for i in range(C - 1, 0, -1):
            settle(end_out, end_send.at[i], {"row": partner}).wait_send()

    if C > 2:
        @pl.when((z > 0) & (z < C - 1))
        def _():
            line_copy(0).wait_send()
            line_copy(1).wait_send()


def hand_over_kernel(*refs):
    n = (len(refs) - 1) // 2
    sources, targets, sems = refs[:n], refs[n:2 * n], refs[-1]
    stores = [pltpu.make_async_copy(sources[i], targets[i], sems.at[i]) for i in range(n)]
    for store in stores:
        store.start()
    for store in stores:
        store.wait()


def per_device(
    tokens,
    frozen_weight,
    input_adapter_factor,
    output_adapter_factor,
    magnitude,
    cotangent,
    sequence_lengths,
):
    D, C, R = lax.axis_size("dp"), lax.axis_size("col"), lax.axis_size("row")
    local_rows, features = tokens.shape
    block_rows, cols = cotangent.shape
    rank_rows = input_adapter_factor.shape[0]
    S, L = 4, 2
    feature_tiles = features // FEATURE_TILE
    sub = local_rows // S
    units = C * S
    block_units = units // R
    g1 = D * R
    vmem = pl.BlockSpec(memory_space=pltpu.VMEM)
    hbm = pl.BlockSpec(memory_space=pl.ANY)
    dma = pltpu.SemaphoreType.DMA
    regular = pltpu.SemaphoreType.REGULAR
    f32, bf16 = jnp.float32, jnp.bfloat16
    results = pl.pallas_call(
        functools.partial(adapter_kernel, D, C, R, S, L),
        out_shape=(
            pltpu.VMEM((block_rows, cols), bf16),
            pltpu.VMEM((1, cols), f32),
            pltpu.VMEM((rank_rows, features), f32),
            pltpu.VMEM((rank_rows, cols), f32),
        ),
        in_specs=[hbm] * 7,
        out_specs=(vmem, vmem, vmem, vmem),
        scratch_shapes=[
            pltpu.SMEM(sequence_lengths.shape, jnp.int32),
            pltpu.VMEM((features, cols), bf16),
            pltpu.VMEM((feature_tiles, cols, features // feature_tiles), bf16),
            pltpu.VMEM((units, sub, features), bf16),
            pltpu.VMEM((units, sub, cols), bf16),
            pltpu.VMEM((units, sub, cols), bf16),
            pltpu.VMEM((R // 2, block_units, sub, cols), bf16),
            pltpu.VMEM((2, sub, cols), f32),
            pltpu.VMEM((R, rank_rows + 8, cols), f32),
            pltpu.VMEM((R // 2, rank_rows + 8, cols), f32),
            pltpu.VMEM((rank_rows, features), bf16),
            pltpu.VMEM((rank_rows, cols), bf16),
            pltpu.VMEM((1, cols), f32),
            pltpu.VMEM((LANES, features), bf16),
            pltpu.VMEM((LANES, cols), bf16),
            pltpu.VMEM((block_units, sub, cols), f32),
            pltpu.VMEM((block_units, sub, cols), f32),
            pltpu.VMEM((block_rows, cols), bf16),
            pltpu.VMEM((block_rows, cols), bf16),
            pltpu.VMEM((L * sub, cols), bf16),
            pltpu.VMEM((block_rows, LANES), f32),
            pltpu.VMEM((L * sub, LANES), f32),
            pltpu.VMEM((R, rank_rows, local_rows), f32),
            pltpu.VMEM((C, rank_rows, local_rows), bf16),
            pltpu.VMEM((rank_rows, cols), f32),
            pltpu.VMEM((1, cols), f32),
            pltpu.VMEM((1, cols), f32),
            pltpu.VMEM((1, cols), f32),
            pltpu.VMEM((g1, 1, cols), f32),
            pltpu.VMEM((R, rank_rows, block_rows), bf16),
            pltpu.VMEM((R, block_rows, LANES), bf16),
            pltpu.VMEM((sub, LANES), bf16),
            pltpu.VMEM((rank_rows, cols), f32),
            pltpu.VMEM((rank_rows, cols), f32),
            pltpu.VMEM((g1, rank_rows, max(LANES, cols // g1)), f32),
            pltpu.VMEM((rank_rows, features), f32),
            pltpu.VMEM((D, rank_rows, features), bf16),
            pltpu.VMEM((rank_rows, features), f32),
            pltpu.VMEM((2, rank_rows, features), bf16),
            pltpu.VMEM((2, rank_rows, features), bf16),
            pltpu.VMEM((feature_tiles, rank_rows, features // feature_tiles), bf16),
            pltpu.VMEM((2, feature_tiles, rank_rows, features // feature_tiles), bf16),
            pltpu.VMEM((rank_rows, LANES), f32),
            pltpu.VMEM((max(2, C - 1), rank_rows, LANES), f32),
            dma((6,)),
            dma((S,)),
            regular,
            pltpu.SemaphoreType.REGULAR((max(1, C - 2),)),
            dma((2,)),
            dma((units,)),
            dma((2,)),
            dma((2, PIECES)),
            dma((2,)),
            dma((R // 2 * block_units,)),
            dma((max(1, R // 2 - 1), block_units)),
            dma((2,)),
            dma((2,)),
            dma(()),
            dma(()),
            dma(()),
            dma(()),
            dma((R // 2,)),
            dma(()),
            dma(()),
            dma(()),
            dma(()),
            dma(()),
            dma(()),
            dma(()),
            dma((2,)),
            dma((2,)),
            dma((C,)),
            dma((2,)),
            dma(()),
            dma(()),
            dma(()),
            dma((2,)),
        ] + [dma(())] * 4,
        compiler_params=pltpu.CompilerParams(
            collective_id=0, has_side_effects=True, vmem_limit_bytes=VMEM_LIMIT
        ),
    )(
        tokens.reshape(S, sub, features), frozen_weight, input_adapter_factor,
        output_adapter_factor, magnitude.reshape(1, cols), cotangent, sequence_lengths,
    )
    results = [pltpu.with_memory_space_constraint(x, pltpu.VMEM) for x in results]
    projected, grad_mag, factor_grad, grad_b = pl.pallas_call(
        hand_over_kernel,
        out_shape=tuple(jax.ShapeDtypeStruct(x.shape, x.dtype) for x in results),
        in_specs=[vmem] * len(results),
        out_specs=(hbm,) * len(results),
        scratch_shapes=[dma((len(results),))],
    )(*results)
    return projected, grad_mag.reshape(cols), factor_grad, grad_b


def solution(mesh):
    in_specs = (
        P(("dp", "col"), "row"),
        P("row", "col"),
        P(None, "row"),
        P(None, "col"),
        P("col"),
        P(("dp", "row"), "col"),
        P("dp", None),
    )
    out_specs = (P(("dp", "row"), "col"), P("col"), P(None, "row"), P(None, "col"))
    return jax.shard_map(
        per_device, mesh=mesh, in_specs=in_specs, out_specs=out_specs, check_vma=False
    )
```

```python
import functools

import jax
import jax.numpy as jnp
from jax import lax
from jax.experimental import pallas as pl
from jax.experimental.pallas import tpu as pltpu
from jax.sharding import PartitionSpec as P

norm_eps = 1e-06
highest_precision = lax.Precision.HIGHEST
MESH = pl.DeviceIdType.MESH
LANES = 128
FEATURE_TILE = 512
TURN = 256
PIECES = 8
VMEM_LIMIT = 56 * 1024 * 1024


def contract_product(left, right, left_dim, right_dim):
    return lax.dot_general(
        left, right, (((left_dim,), (right_dim,)), ((), ())), preferred_element_type=jnp.float32
    )


def column_tiles(width, tile):
    return [(start, min(tile, width - start)) for start in range(0, width, tile)]


def adapter_kernel(
    D, C, R, S, L,
    tok, w_hbm, a_hbm, b_hbm, magnitude_hbm, cot_hbm, lengths_hbm,
    projected, grad_mag, factor_grad, grad_b,
    lengths, wx, wt, gath, sb, pin, xin, pb, st_in, st_pair, a_ref, b_ref, magnitude, apad, bpad, acc, own_sum, pg, cot, late_cot,
    row_weight, late_weight, down_in, down_all, merged_factor, col_norm, col_scale, coefficient_scale,
    scale_in, back_in, back_rows, back_far, bsum, bsum_all, box1, fsum, fsum_in, message, line_in, line_out, end_out, end_in, cross_out, cross_in,
    load_sem, tok_sem, plane_sem, line_sem, gsend, grecv, qsend, qrecv, ssend, precv, xrecv, stsend, strecv,
    dn_send, dn_recv, dz_send, dz_recv, late_send, late_recv, sc_send, sc_recv, bk_send, bk_recv,
    fs_send, fs_recv, ln_send, ln_recv, end_send, end_recv, bf_send, bf_recv, cx_send, cx_recv, r1a, r1b, r1c, r1d,
):
    z = lax.axis_index("col")
    r = lax.axis_index("row")
    d = lax.axis_index("dp")
    p, q = r // 2, r % 2
    pairs = R // 2
    sub, features = tok.shape[1], tok.shape[2]
    cols = w_hbm.shape[1]
    rank_rows = a_ref.shape[0]
    units = C * S
    block_units = units // R
    block_rows = block_units * sub
    chunks = block_units // S
    tiles = column_tiles(cols, 512)
    feature_tiles = column_tiles(features, FEATURE_TILE)
    f32, bf16 = jnp.float32, jnp.bfloat16
    half = units // 2
    catch_up = half + 3
    rate = 4

    g1 = D * R
    me1 = d * R + r

    def device1(i):
        peer = (me1 + i) % g1
        return {"dp": peer // R, "row": peer % R}

    def loop(n, body):
        def turn(i, carry):
            body(i)
            return carry

        lax.fori_loop(1, n, turn, 0)

    def remote(src, dst, send_sem, recv_sem, device):
        return pltpu.make_async_remote_copy(
            src_ref=src, dst_ref=dst, send_sem=send_sem, recv_sem=recv_sem,
            device_id=device, device_id_type=MESH,
        )

    def settle(view, sem, device):
        return remote(view, view, sem, sem, device)

    def signal(sem, device):
        pl.semaphore_signal(sem, inc=1, device_id=device, device_id_type=MESH)

    def signal_line(sem):
        @pl.when(z > 0)
        def _():
            signal(sem, {"col": z - 1})

        @pl.when(z < C - 1)
        def _():
            signal(sem, {"col": z + 1})

    line_count = jnp.where(z > 0, 1, 0) + jnp.where(z < C - 1, 1, 0)

    barrier = pltpu.get_barrier_semaphore()
    signal_line(barrier)
    for i in range(1, R):
        signal(barrier, {"row": (r + i) % R})
    for i in range(1, D):
        signal(barrier, {"dp": (d + i) % D})

    def load_tok(s):
        return pltpu.make_async_copy(tok.at[s], gath.at[z * S + s], tok_sem.at[s])

    small_loads = [
        pltpu.make_async_copy(a_hbm, a_ref, load_sem.at[0]),
        pltpu.make_async_copy(b_hbm, b_ref, load_sem.at[1]),
        pltpu.make_async_copy(magnitude_hbm, magnitude, load_sem.at[2]),
        pltpu.make_async_copy(lengths_hbm, lengths, load_sem.at[5]),
    ]
    load_w = pltpu.make_async_copy(w_hbm, wx, load_sem.at[3])
    load_c = pltpu.make_async_copy(cot_hbm, cot, load_sem.at[4])
    for s in range(S):
        load_tok(s).start()
    for load in small_loads:
        load.start()
    load_w.start()
    load_c.start()

    pl.semaphore_wait(barrier, line_count + R - 1 + D - 1)

    def hop(u, direction):
        target = z - 1 if direction == 0 else z + 1
        return remote(gath.at[u], gath.at[u], gsend.at[direction], grecv.at[u], {"col": target})

    ends = (z == 0) | (z == C - 1)
    piece = features // PIECES

    def hop_piece(u, j):
        view = gath.at[u, :, pl.ds(j * piece, piece)]
        origin = jnp.where(u // S == 0, 0, 1)
        target = jnp.clip(jnp.where(u // S == 0, z + 1, z - 1), 0, C - 1)
        return remote(view, view, qsend.at[origin], qrecv.at[origin, j], {"col": target})

    for s in range(S):
        load_tok(s).wait()
        whole = jnp.logical_not(ends) if s == S - 1 else True

        @pl.when((z > 0) & whole)
        def _():
            hop(z * S + s, 0).start()

        @pl.when((z < C - 1) & whole)
        def _():
            hop(z * S + s, 1).start()

    @pl.when(ends)
    def _():
        for j in range(PIECES):
            hop_piece(z * S + S - 1, j).start()

    for i in range(1, D):
        signal(plane_sem, {"dp": (d + i) % D})
    for load in small_loads:
        load.wait()

    def down_copy(i, piece):
        return remote(
            down_in.at[piece], down_in.at[piece], dn_send, dn_recv, {"row": (r + i) % R}
        )

    def spread_copy(i, piece):
        return remote(
            down_all.at[piece], down_all.at[piece], dz_send, dz_recv, {"col": (z + i) % C}
        )

    a = a_ref[...]
    own_tokens = gath[pl.ds(z * S, S)].reshape(S * sub, features)
    down_in[r] = contract_product(a, own_tokens, 1, 1)
    for i in range(1, R):
        down_copy(i, r).start()
    apad[...] = jnp.zeros_like(apad)
    bpad[...] = jnp.zeros_like(bpad)
    apad[0:rank_rows, :] = a
    bpad[0:rank_rows, :] = b_ref[...]
    if C > 2:
        signal_line(line_sem.at[0])

    far_chunk = jnp.where(z > C - 1 - z, 0, C - 1)
    late_first = far_chunk * S + S - L
    late_owner = late_first // block_units
    late_slot = late_first % block_units

    def weights_of(first, rows):
        position = first + lax.broadcasted_iota(jnp.int32, (rows, LANES), 0)
        weights = jnp.zeros((rows, LANES), f32)
        start_row = 0
        for i in range(lengths.shape[1]):
            length = lengths[0, i]
            end_row = start_row + length
            inverse = 1.0 / jnp.full((1, LANES), length, jnp.int32).astype(f32)
            weights = jnp.where((position >= start_row) & (position < end_row), inverse, weights)
            start_row = end_row
        return weights

    row_weight[...] = weights_of(r * block_rows, block_rows)
    late_weight[...] = weights_of(late_first * sub, L * sub)

    load_w.wait()

    gram = contract_product(a, a, 1, 1)
    for start, width in tiles:
        span = pl.ds(start, width)
        st_in[r, 0:rank_rows, span] = jnp.dot(
            a, wx[:, span], preferred_element_type=f32
        ) + jnp.dot(
            gram, b_ref[:, span].astype(f32),
            precision=highest_precision, preferred_element_type=f32,
        )
        st_in[r, rank_rows:rank_rows + 8, span] = jnp.zeros((8, width), f32)
    depth = 256

    def norm_step(i, carry):
        rows = pl.ds(pl.multiple_of(i * depth, depth), depth)
        for start, width in tiles:
            span = pl.ds(start, width)
            merged = wx[rows, span].astype(f32) + contract_product(apad[:, rows], bpad[:, span], 0, 0)
            st_in[r, rank_rows:rank_rows + 1, span] += jnp.sum(merged * merged, axis=0, keepdims=True)
        return carry

    lax.fori_loop(0, features // depth, norm_step, 0)

    partner = p * 2 + (1 - q)

    def stat_near():
        return remote(st_in.at[r], st_in.at[r], stsend.at[0], strecv.at[0], {"row": partner})

    def stat_far(i, piece):
        return remote(
            st_pair.at[piece], st_pair.at[piece], stsend.at[1], strecv.at[1],
            {"row": ((p + i) % pairs) * 2 + q},
        )

    stat_near().start()

    def pair_stats():
        remote(st_in.at[partner], st_in.at[partner], stsend.at[0], strecv.at[0], {"row": partner}).wait_recv()
        st_pair[p] = st_in[r] + st_in[partner]
        for i in range(1, pairs):
            stat_far(i, p).start()

    def greet():
        pl.semaphore_wait(line_sem.at[0], line_count)
        for i in range(1, C - 2):
            signal_line(line_sem.at[i])
            if i < C - 3:
                pl.semaphore_wait(line_sem.at[i], line_count)

    def spread_down():
        if C > 3:
            pl.semaphore_wait(line_sem.at[C - 3], line_count)
        settle(down_in.at[pl.ds(0, R - 1)], dn_recv, {"row": partner}).wait_recv()
        down = down_in[0]
        for i in range(1, R):
            down = down + down_in[i]
        down_all[z] = down.astype(bf16)
        @pl.when(r == z * S // block_units)
        def _():
            loop(C, lambda i: spread_copy(i, z).start())

    near = jnp.minimum(z, C - 1 - z)

    def place(k):
        j = k - S
        both = j < 2 * near * S
        rest = j - 2 * near * S
        distance = jnp.where(both, j // (2 * S) + 1, near + 1 + rest // S)
        s = jnp.where(both, (j % (2 * S)) // 2, rest % S)
        leftward = jnp.where(both, j % 2 == 0, z > C - 1 - z)
        chunk = jnp.where(leftward, z - distance, z + distance)
        own = k < S
        return jnp.where(own, z, chunk), jnp.where(own, k, s)

    def unit_of(k):
        c, s = place(k)
        return c * S + s

    def pair_copy(u):
        slot = u // block_units // 2 * block_units + u % block_units
        return remote(sb.at[u], pin.at[u], ssend.at[0], precv.at[slot], {"row": p * 2 + (1 - q)})

    def far_copy(u, owner_pair):
        return remote(
            sb.at[u], xin.at[p, u % block_units], ssend.at[1],
            xrecv.at[(p - owner_pair + pairs) % pairs - 1, u % block_units],
            {"row": owner_pair * 2 + q},
        )

    late_pair, late_core = late_owner // 2, late_owner % 2

    def late_far(i):
        rows = pl.ds(pl.multiple_of(late_slot * sub, sub), L * sub)
        return remote(cot.at[rows], late_cot, late_send.at[i], late_recv, {"row": ((p + i) % pairs) * 2 + q})

    def late_near():
        return remote(late_cot, late_cot, late_send.at[0], late_recv, {"row": partner})

    def back_copy(i, piece):
        return remote(back_in.at[piece], back_in.at[piece], bk_send, bk_recv, {"row": (r + i) % R})

    def far_back_copy():
        unit = far_chunk * S + S - 1
        rows = pl.ds(pl.multiple_of(unit % block_units * sub, sub), sub)
        return remote(back_rows.at[unit // block_units, rows, :], back_far, bf_send, bf_recv, {"col": C - 1 - z})

    def scale_copy(i, piece):
        return remote(scale_in.at[piece], scale_in.at[piece], sc_send, sc_recv, device1(i))

    def group_sum(g, me, device, src, box, out, s1, r1, s2, r2):
        width = max(LANES, src.shape[1] // g)
        pieces = src.shape[1] // width

        def part(j):
            return pl.ds(pl.multiple_of(j * width, width), width)

        def scatter(i):
            return remote(src.at[:, part((me + i) % g % pieces)], box.at[i], s1, r1, device(i))

        def spread(i, j):
            return remote(out.at[:, part(j % pieces)], out.at[:, part(j % pieces)], s2, r2, device(i))

        def await_pieces(count, sem, sent):
            if count > 0:
                copies = settle(box.at[pl.ds(0, count)], sem, device(1))
                copies.wait_send() if sent else copies.wait_recv()

        def await_owners(sem, sent):
            if pieces == g:
                await_pieces(pieces - 1, sem, sent)
            else:
                @pl.when(me < pieces)
                def _():
                    await_pieces(pieces - 1, sem, sent)

                @pl.when(me >= pieces)
                def _():
                    await_pieces(pieces, sem, sent)

        def begin():
            def send(i):
                @pl.when((me + i) % g < pieces)
                def _():
                    scatter(i).start()

            loop(g, send)

        def middle():
            @pl.when(me < pieces)
            def _():
                await_pieces(g - 1, r1, False)
                out[:, part(me % pieces)] = lax.fori_loop(
                    1, g, lambda i, total: total + box[i], src[:, part(me % pieces)]
                )
                loop(g, lambda i: spread(i, me).start())

        def end():
            await_owners(r2, False)

        def drain():
            await_owners(s1, True)

            @pl.when(me < pieces)
            def _():
                await_pieces(g - 1, s2, True)

        return begin, middle, end, drain

    begin1, middle1, end1, drain1 = group_sum(
        g1, me1, device1, bsum, box1, bsum_all, r1a, r1b, r1c, r1d
    )

    def early():
        if pairs > 1:
            settle(st_pair.at[pl.ds(0, pairs - 1)], strecv.at[1], {"row": partner}).wait_recv()
        stats = st_pair[0]
        for i in range(1, pairs):
            stats = stats + st_pair[i]
        merged_factor[...] = stats[0:rank_rows]
        norm = jnp.sqrt(stats[rank_rows:rank_rows + 1] + norm_eps)
        col_norm[...] = norm
        col_scale[...] = magnitude[...] / norm
        coefficient_scale[...] = -magnitude[...] / (norm * norm * norm)
        load_c.wait()
        scale_in[me1] = jnp.zeros((1, cols), f32)
        for v in range(block_units):
            rows = pl.ds(v * sub, sub)
            weight = row_weight[rows, 0:1]
            for start, width in tiles:
                span = pl.ds(start, width)
                grad_out = cot[rows, span].astype(f32) * weight
                pg[rows, span] = (grad_out * col_scale[:, span]).astype(bf16)
        back_in[r] = contract_product(b_ref[...], pg[...], 1, 1).astype(bf16)
        for i in range(1, R):
            back_copy(i, r).start()

    def middle():
        @pl.when(z // chunks != r)
        def _():
            settle(down_all.at[pl.ds(0, chunks)], dz_recv, {"row": partner}).wait_recv()

        if chunks > 1:
            @pl.when(z // chunks == r)
            def _():
                settle(down_all.at[pl.ds(0, chunks - 1)], dz_recv, {"row": partner}).wait_recv()

        for start, width in tiles:
            span = pl.ds(start, width)
            total = jnp.zeros((rank_rows, width), f32)
            for i in range(chunks):
                down = down_all[r * chunks + i]
                total = total + jnp.dot(
                    down, pg[i * S * sub:(i + 1) * S * sub, span], preferred_element_type=f32
                )
                acc[i * S:(i + 1) * S, :, span] = contract_product(
                    down, b_ref[:, span], 0, 0
                ).reshape(S, sub, width)
            bsum[:, span] = total
        if D > 1:
            pl.semaphore_wait(plane_sem, D - 1)
        begin1()

        @pl.when(r == late_owner)
        def _():
            for i in range(L):
                rows = pl.ds(pl.multiple_of((late_slot + i) * sub, sub), sub)
                weight = row_weight[rows, 0:1]
                for start, width in tiles:
                    span = pl.ds(start, width)
                    grad_out = cot[rows, span].astype(f32) * weight
                    scale_in[me1, :, span] += jnp.sum(
                        grad_out * acc[late_slot + i, :, span], axis=0, keepdims=True
                    )

    def send_late():
        @pl.when(r == late_owner)
        def _():
            for i in range(1, pairs):
                late_far(i).start()
            late_cot[...] = cot[pl.ds(pl.multiple_of(late_slot * sub, sub), L * sub), :]

    def pass_late():
        @pl.when(q == late_core)
        def _():
            @pl.when(p != late_pair)
            def _():
                late_near().wait_recv()

            late_near().start()

    def multiply(k):
        c, s = place(k)
        u = c * S + s
        owner = u // block_units

        split = (k >= S) & (s == S - 1) & ((c == 0) | (c == C - 1))

        @pl.when((k >= S) & jnp.logical_not(split))
        def _():
            hop(u, 0).wait_recv()

            @pl.when((c < z) & (z < C - 1))
            def _():
                hop(u, 1).start()

            @pl.when((c > z) & (z > 0))
            def _():
                hop(u, 0).start()

        slot = k % 2

        @pl.when(jnp.logical_not(split))
        def _():
            for start, width in tiles:
                span = pl.ds(start, width)
                pb[slot, :, span] = jnp.dot(gath[u], wx[:, span], preferred_element_type=f32)

        @pl.when(split)
        def _():
            for j in range(PIECES):
                hop_piece(u, j).wait_recv()

                @pl.when(((c == 0) & (z < C - 1)) | ((c != 0) & (z > 0)))
                def _():
                    hop_piece(u, j).start()

                part = pl.ds(j * piece, piece)
                for start, width in tiles:
                    span = pl.ds(start, width)
                    product = jnp.dot(gath[u, :, part], wx[part, span], preferred_element_type=f32)
                    pb[slot, :, span] = product if j == 0 else pb[slot, :, span] + product

        @pl.when(k >= units - L)
        def _():
            @pl.when((k == units - L) & (q != late_core))
            def _():
                late_near().wait_recv()

            rows = pl.ds(pl.multiple_of((k - units + L) * sub, sub), sub)
            weight = late_weight[rows, 0:1]
            for start, width in tiles:
                span = pl.ds(start, width)
                grad_out = late_cot[rows, span].astype(f32) * weight
                scale_in[me1, :, span] += jnp.sum(grad_out * pb[slot, :, span], axis=0, keepdims=True)

        @pl.when(k == units - 1)
        def _():
            loop(g1, lambda i: scale_copy(i, me1).start())

        @pl.when(owner % 2 != q)
        def _():
            sb[u] = pb[slot].astype(bf16)
            pair_copy(u).start()

    def combine(k):
        u = unit_of(k)
        owner = u // block_units
        slot = k % 2

        @pl.when(owner % 2 == q)
        def _():
            pair_copy(u).wait_recv()
            total = pb[slot] + pin[u].astype(f32)

            @pl.when(owner // 2 == p)
            def _():
                own_sum[u % block_units] = total

            @pl.when(owner // 2 != p)
            def _():
                sb[u] = total.astype(bf16)
                far_copy(u, owner // 2).start()

    def factor_term(k):
        u = unit_of(k)
        block = u // block_units
        rows = pl.ds(pl.multiple_of((u % block_units) * sub, sub), sub)
        add_term(u, back_rows[block, rows, :])

    def add_term(u, back):
        for start, width in feature_tiles:
            span = pl.ds(start, width)
            fsum[:, span] += contract_product(back, gath[u, :, span], 0, 0)[0:rank_rows]

    def finish(k):
        u = unit_of(k)

        @pl.when(u // block_units == r)
        def _():
            v = u % block_units
            for i in range(1, pairs):
                other = (p + i) % pairs
                remote(
                    sb.at[v], xin.at[other, v], ssend.at[1], xrecv.at[i - 1, v], {"row": other * 2 + q}
                ).wait_recv()
            rows = pl.ds(pl.multiple_of(v * sub, sub), sub)
            weight = row_weight[rows, 0:1]
            for start, width in tiles:
                span = pl.ds(start, width)
                query = acc[v, :, span] + own_sum[v, :, span]
                for i in range(1, pairs):
                    query = query + xin[(p + i) % pairs, v, :, span].astype(f32)
                projected[rows, span] = (query * col_scale[:, span]).astype(bf16)
                grad_out = cot[rows, span].astype(f32) * weight

                @pl.when(k < units - L)
                def _():
                    scale_in[me1, :, span] += jnp.sum(grad_out * query, axis=0, keepdims=True)

    def each(first, last, body):
        def turn(i, carry):
            body(i)
            return carry

        lax.fori_loop(first, last, turn, 0)

    def group_copy(i, piece):
        return remote(fsum_in.at[piece], fsum_in.at[piece], fs_send, fs_recv, {"dp": (d + i) % D})

    def share_term():
        fsum_in[d] = fsum[...].astype(bf16)
        for i in range(1, D):
            group_copy(i, d).start()

    fsum[...] = jnp.zeros_like(fsum)
    cross_out[...] = jnp.zeros_like(cross_out)

    def step(k, carry):
        @pl.when(k > 0)
        def _():
            combine(k - 1)

        @pl.when(k == 1)
        def _():
            pair_stats()

        turned = k - (units - 1 - features // TURN)

        @pl.when(ends & (turned >= 0) & (turned < features // TURN))
        def _():
            per_tile = FEATURE_TILE // TURN
            rows = pl.ds(pl.multiple_of(turned * TURN, TURN), TURN)
            lanes = pl.ds(pl.multiple_of(turned % per_tile * TURN, TURN), TURN)
            wt[turned // per_tile, :, lanes] = wx[rows, :].T

        if C > 2:
            @pl.when(k == 2)
            def _():
                greet()

        @pl.when(k == S)
        def _():
            spread_down()

        @pl.when(k == half)
        def _():
            early()

        @pl.when(k == half + 1)
        def _():
            send_late()

        @pl.when(k == half + 2)
        def _():
            middle()

        @pl.when(k == catch_up)
        def _():
            settle(back_in.at[pl.ds(0, R - 1)], bk_recv, {"row": partner}).wait_recv()
            one = (
                lax.broadcasted_iota(jnp.int32, (rank_rows, LANES), 0)
                == lax.broadcasted_iota(jnp.int32, (rank_rows, LANES), 1)
            ).astype(f32).astype(bf16)
            for j in range(R):
                back_rows[j] = contract_product(back_in[j], one, 0, 0).astype(bf16)

            @pl.when(z == C - 1)
            def _():
                far_back_copy().start()

        @pl.when(k >= catch_up)
        def _():
            done = rate * (k - catch_up)
            each(jnp.minimum(done, k - 1), jnp.minimum(done + rate, k), factor_term)
            each(jnp.minimum(done, k - 2), jnp.minimum(done + rate, k - 1), finish)

        @pl.when((k == units - 2) & (z == 0))
        def _():
            far_back_copy().wait_recv()
            add_term(z * S + S - 1, back_far[...])

        @pl.when((k == units - 1) & (z == C - 1))
        def _():
            share_term()

        @pl.when(k == catch_up + 1)
        def _():
            pass_late()

        @pl.when(k == units - 2)
        def _():
            middle1()

        multiply(k)
        return carry

    lax.fori_loop(0, units, step, 0)

    @pl.when(z != C - 1)
    def _():
        factor_term(units - 1)
        share_term()

    combine(units - 1)

    side = jnp.where(z == 0, 0, 1)

    def end_copy(i, t):
        target = jnp.where(z == 0, i, C - 1 - i)
        return remote(end_out.at[t], end_in.at[side, t], end_send.at[i], end_recv.at[side], {"col": target})

    def end_arrived(j):
        settle(end_in.at[j], end_recv.at[j], {"row": partner}).wait_recv()
        for t, (start, width) in enumerate(feature_tiles):
            message[:, pl.ds(start, width)] += end_in[j, t].astype(f32)

    def line_copy(direction):
        target = z - 1 if direction == 0 else z + 1
        return remote(
            line_out.at[direction], line_in.at[direction], ln_send.at[direction], ln_recv.at[direction],
            {"col": target},
        )

    settle(scale_in.at[pl.ds(0, g1 - 1)], sc_recv, device1(1)).wait_recv()
    scale_grad = scale_in[0]
    for j in range(1, g1):
        scale_grad = scale_grad + scale_in[j]
    coefficient = scale_grad * coefficient_scale[...]
    scaled = (b_ref[...].astype(f32) * coefficient).astype(bf16)
    if D > 1:
        settle(fsum_in.at[pl.ds(0, D - 1)], fs_recv, {"row": partner}).wait_recv()

    def term(t, product):
        start, width = feature_tiles[t]
        span = pl.ds(start, width)
        total = product + fsum[:, span]
        for i in range(1, D):
            total = total + fsum_in[(d - i + D) % D, :, span].astype(f32)
        message[:, span] = total
        return total

    def add_cross(cross):
        for start, width in feature_tiles:
            span = pl.ds(start, width)
            message[:, span] += jnp.dot(
                cross, a_ref[:, span].astype(f32),
                precision=highest_precision, preferred_element_type=f32,
            )

    def cross_copy(i):
        target = jnp.where(z == 0, i, C - 1 - i)
        return remote(cross_out, cross_in.at[side], cx_send, cx_recv.at[side], {"col": target})

    @pl.when(ends)
    def _():
        for t in range(len(feature_tiles)):
            end_out[t] = term(t, jnp.dot(scaled, wt[t], preferred_element_type=f32)).astype(bf16)
            end_copy(C - 1, t).start()
            if t == 0:
                cross_out[:, 0:rank_rows] = contract_product(scaled, b_ref[...], 1, 1)
                for i in range(C - 1, 0, -1):
                    cross_copy(i).start()
        for i in range(C - 2, 0, -1):
            for t in range(len(feature_tiles)):
                end_copy(i, t).start()

    @pl.when(jnp.logical_not(ends))
    def _():
        for t, (start, width) in enumerate(feature_tiles):
            term(t, contract_product(scaled, wx[pl.ds(start, width), :], 1, 1))
        add_cross(contract_product(scaled, b_ref[...], 1, 1))

    def drain_stream(direction):
        for i in range(C):
            count = (C - i) * S - 1 if direction == 0 else (i + 1) * S - 1
            if 0 <= i + 2 * direction - 1 < C:
                @pl.when(z == i)
                def _():
                    settle(gath.at[pl.ds(0, count)], gsend.at[direction], {"row": partner}).wait_send()
                    settle(gath.at[0], qsend.at[1 - direction], {"row": partner}).wait_send()

    if C > 2:
        @pl.when((z > 0) & (z < C - 1))
        def _():
            own = message[...]
            more = ((z < C - 2), (z > 1))
            for direction in (0, 1):
                @pl.when(jnp.logical_not(more[direction]))
                def _():
                    line_out[direction] = own.astype(bf16)
                    drain_stream(direction)
                    line_copy(direction).start()

            for direction in (0, 1):
                @pl.when(more[direction])
                def _():
                    line_copy(direction).wait_recv()
                    incoming = line_in[direction].astype(f32)
                    line_out[direction] = (own + incoming).astype(bf16)
                    message[...] += incoming
                    drain_stream(direction)
                    line_copy(direction).start()

    each(units - 2, units, finish)
    grad_mag[...] = scale_grad / col_norm[...]
    end1()
    grad_b[...] = bsum_all[...] + merged_factor[...] * coefficient

    drain1()
    settle(scale_in.at[pl.ds(0, g1 - 1)], sc_send, device1(1)).wait_send()
    settle(back_in.at[pl.ds(0, R - 1)], bk_send, {"row": partner}).wait_send()
    settle(down_in.at[pl.ds(0, R - 1)], dn_send, {"row": partner}).wait_send()

    @pl.when(r == z * S // block_units)
    def _():
        settle(down_all.at[pl.ds(0, C - 1)], dz_send, {"row": partner}).wait_send()

    if D > 1:
        settle(fsum_in.at[pl.ds(0, D - 1)], fs_send, {"row": partner}).wait_send()

    stat_near().wait_send()
    if pairs > 1:
        settle(st_pair.at[pl.ds(0, pairs - 1)], stsend.at[1], {"row": partner}).wait_send()

    @pl.when(r == late_owner)
    def _():
        for i in range(1, pairs):
            late_far(i).wait_send()

    @pl.when(q == late_core)
    def _():
        late_near().wait_send()

    settle(sb.at[pl.ds(0, units // 2)], ssend.at[0], {"row": partner}).wait_send()
    if pairs > 1:
        settle(sb.at[pl.ds(0, block_units * (pairs - 1))], ssend.at[1], {"row": partner}).wait_send()

    @pl.when(ends)
    def _():
        drain_stream(0)
        drain_stream(1)


    if C > 2:
        @pl.when(z == 0)
        def _():
            line_copy(0).wait_recv()
            message[...] += line_in[0].astype(f32)

        @pl.when(z == C - 1)
        def _():
            line_copy(1).wait_recv()
            message[...] += line_in[1].astype(f32)

    for j in (0, 1):
        @pl.when(z != j * (C - 1))
        def _():
            remote(cross_out, cross_in.at[j], cx_send, cx_recv.at[j], {"row": partner}).wait_recv()
            add_cross(cross_in[j, :, 0:rank_rows])

    @pl.when(ends)
    def _():
        add_cross(cross_out[:, 0:rank_rows])

    @pl.when(z > 0)
    def _():
        end_arrived(0)

    @pl.when(z < C - 1)
    def _():
        end_arrived(1)

    factor_grad[...] = message[...]

    @pl.when(ends)
    def _():
        @pl.when(z == C - 1)
        def _():
            far_back_copy().wait_send()

        settle(cross_in.at[pl.ds(0, C - 1)], cx_send, {"row": partner}).wait_send()
        for i in range(C - 1, 0, -1):
            settle(end_out, end_send.at[i], {"row": partner}).wait_send()

    if C > 2:
        @pl.when((z > 0) & (z < C - 1))
        def _():
            line_copy(0).wait_send()
            line_copy(1).wait_send()


def hand_over_kernel(*refs):
    n = (len(refs) - 1) // 2
    sources, targets, sems = refs[:n], refs[n:2 * n], refs[-1]
    stores = [pltpu.make_async_copy(sources[i], targets[i], sems.at[i]) for i in range(n)]
    for store in stores:
        store.start()
    for store in stores:
        store.wait()


def per_device(
    tokens,
    frozen_weight,
    input_adapter_factor,
    output_adapter_factor,
    magnitude,
    cotangent,
    sequence_lengths,
):
    D, C, R = lax.axis_size("dp"), lax.axis_size("col"), lax.axis_size("row")
    local_rows, features = tokens.shape
    block_rows, cols = cotangent.shape
    rank_rows = input_adapter_factor.shape[0]
    S, L = 4, 2
    feature_tiles = features // FEATURE_TILE
    sub = local_rows // S
    units = C * S
    block_units = units // R
    g1 = D * R
    vmem = pl.BlockSpec(memory_space=pltpu.VMEM)
    hbm = pl.BlockSpec(memory_space=pl.ANY)
    dma = pltpu.SemaphoreType.DMA
    regular = pltpu.SemaphoreType.REGULAR
    f32, bf16 = jnp.float32, jnp.bfloat16
    results = pl.pallas_call(
        functools.partial(adapter_kernel, D, C, R, S, L),
        out_shape=(
            pltpu.VMEM((block_rows, cols), bf16),
            pltpu.VMEM((1, cols), f32),
            pltpu.VMEM((rank_rows, features), f32),
            pltpu.VMEM((rank_rows, cols), f32),
        ),
        in_specs=[hbm] * 7,
        out_specs=(vmem, vmem, vmem, vmem),
        scratch_shapes=[
            pltpu.SMEM(sequence_lengths.shape, jnp.int32),
            pltpu.VMEM((features, cols), bf16),
            pltpu.VMEM((feature_tiles, cols, features // feature_tiles), bf16),
            pltpu.VMEM((units, sub, features), bf16),
            pltpu.VMEM((units, sub, cols), bf16),
            pltpu.VMEM((units, sub, cols), bf16),
            pltpu.VMEM((R // 2, block_units, sub, cols), bf16),
            pltpu.VMEM((2, sub, cols), f32),
            pltpu.VMEM((R, rank_rows + 8, cols), f32),
            pltpu.VMEM((R // 2, rank_rows + 8, cols), f32),
            pltpu.VMEM((rank_rows, features), bf16),
            pltpu.VMEM((rank_rows, cols), bf16),
            pltpu.VMEM((1, cols), f32),
            pltpu.VMEM((LANES, features), bf16),
            pltpu.VMEM((LANES, cols), bf16),
            pltpu.VMEM((block_units, sub, cols), f32),
            pltpu.VMEM((block_units, sub, cols), f32),
            pltpu.VMEM((block_rows, cols), bf16),
            pltpu.VMEM((block_rows, cols), bf16),
            pltpu.VMEM((L * sub, cols), bf16),
            pltpu.VMEM((block_rows, LANES), f32),
            pltpu.VMEM((L * sub, LANES), f32),
            pltpu.VMEM((R, rank_rows, local_rows), f32),
            pltpu.VMEM((C, rank_rows, local_rows), bf16),
            pltpu.VMEM((rank_rows, cols), f32),
            pltpu.VMEM((1, cols), f32),
            pltpu.VMEM((1, cols), f32),
            pltpu.VMEM((1, cols), f32),
            pltpu.VMEM((g1, 1, cols), f32),
            pltpu.VMEM((R, rank_rows, block_rows), bf16),
            pltpu.VMEM((R, block_rows, LANES), bf16),
            pltpu.VMEM((sub, LANES), bf16),
            pltpu.VMEM((rank_rows, cols), f32),
            pltpu.VMEM((rank_rows, cols), f32),
            pltpu.VMEM((g1, rank_rows, max(LANES, cols // g1)), f32),
            pltpu.VMEM((rank_rows, features), f32),
            pltpu.VMEM((D, rank_rows, features), bf16),
            pltpu.VMEM((rank_rows, features), f32),
            pltpu.VMEM((2, rank_rows, features), bf16),
            pltpu.VMEM((2, rank_rows, features), bf16),
            pltpu.VMEM((feature_tiles, rank_rows, features // feature_tiles), bf16),
            pltpu.VMEM((2, feature_tiles, rank_rows, features // feature_tiles), bf16),
            pltpu.VMEM((rank_rows, LANES), f32),
            pltpu.VMEM((max(2, C - 1), rank_rows, LANES), f32),
            dma((6,)),
            dma((S,)),
            regular,
            pltpu.SemaphoreType.REGULAR((max(1, C - 2),)),
            dma((2,)),
            dma((units,)),
            dma((2,)),
            dma((2, PIECES)),
            dma((2,)),
            dma((R // 2 * block_units,)),
            dma((max(1, R // 2 - 1), block_units)),
            dma((2,)),
            dma((2,)),
            dma(()),
            dma(()),
            dma(()),
            dma(()),
            dma((R // 2,)),
            dma(()),
            dma(()),
            dma(()),
            dma(()),
            dma(()),
            dma(()),
            dma(()),
            dma((2,)),
            dma((2,)),
            dma((C,)),
            dma((2,)),
            dma(()),
            dma(()),
            dma(()),
            dma((2,)),
        ] + [dma(())] * 4,
        compiler_params=pltpu.CompilerParams(
            collective_id=0, has_side_effects=True, vmem_limit_bytes=VMEM_LIMIT
        ),
    )(
        tokens.reshape(S, sub, features), frozen_weight, input_adapter_factor,
        output_adapter_factor, magnitude.reshape(1, cols), cotangent, sequence_lengths,
    )
    results = [pltpu.with_memory_space_constraint(x, pltpu.VMEM) for x in results]
    projected, grad_mag, factor_grad, grad_b = pl.pallas_call(
        hand_over_kernel,
        out_shape=tuple(jax.ShapeDtypeStruct(x.shape, x.dtype) for x in results),
        in_specs=[vmem] * len(results),
        out_specs=(hbm,) * len(results),
        scratch_shapes=[dma((len(results),))],
    )(*results)
    return projected, grad_mag.reshape(cols), factor_grad, grad_b


def solution(mesh):
    in_specs = (
        P(("dp", "col"), "row"),
        P("row", "col"),
        P(None, "row"),
        P(None, "col"),
        P("col"),
        P(("dp", "row"), "col"),
        P("dp", None),
    )
    out_specs = (P(("dp", "row"), "col"), P("col"), P(None, "row"), P(None, "col"))
    return jax.shard_map(
        per_device, mesh=mesh, in_specs=in_specs, out_specs=out_specs, check_vma=False
    )
```
